256 devices in a mesh: section: 4 (over z_hi, core), dp: 64 (over x, y, z_lo).
Axes of the slice: x: 4, y: 4, z: 8 (z_hi: 2, z_lo: 4; z = z_hi * 4 + z_lo), core: 2. Of those that a mesh axis runs over, the one named last changes fastest.
Arguments:
- latent_states: bfloat16 [4, 256, 96, 2048], P('section', 'dp'), may hold values from -8 to 8
- rescale_factor: float32 [2048], replicated, may hold values from 0.25 to 1.75
- embedding_matrix: bfloat16 [2048, 128], P('section'), may hold values from -0.125 to 0.125
- request_span: int32 [4, 256], replicated, may hold values from 8 to 32
- passage_span: int32 [4, 256], replicated, may hold values from 32 to 64
- matching_pair: int32 [4, 256], replicated, may hold values from 0 to 255, each once within a row
- steepness_pair: float32 [2], replicated, may hold values from 8 to 400
Outputs:
- grad_hidden: bfloat16 [4, 256, 96, 2048], P('section', 'dp')
- pair_loss: float32 [4, 256], P('section', 'dp')
The draws below stay inside these ranges and needn't reach their ends.
Inputs may be any that keep to these rules, and one draw needn't show every extreme that they name: Each matching_pair[m] names every pair of the micro-batch once.
All inputs are finite; a program needn't handle non-finite values.
Results may differ from the reference program's by a relative error of at most 0.006.
The reference program's roundings to bfloat16 on the way count: a program that leaves them out, or rounds other values in their place, can miss the bound.
Values may be sent and summed in bfloat16 or wider, within the bound.
No kernel may reach another device: no remote copies, remote signals or barrier semaphores. Data moves between devices by JAX's collectives and lax.ppermute only.
A program may use at most 64 MiB of HBM per device.

```python
import jax
import jax.numpy as jnp
from jax import lax

D = 2048
E = 128
QLEN = 32
DLEN = 64
MICRO = 4
PAIRS_ALL = 256


def draw_latent_states(key, part):
    shape = (MICRO, PAIRS_ALL, QLEN + DLEN, D)
    keys = jax.random.split(jax.random.fold_in(key, 11), 1)
    base = jnp.clip(jax.random.normal(keys[0], shape, jnp.float32), -6.0, 6.0)
    return base.astype(jnp.bfloat16)


def draw_steepness_pair(key, part):
    first_key, latter_seed = jax.random.split(jax.random.fold_in(key, 23))
    pooling_steepness = jax.random.uniform(first_key, (), jnp.float32, 8.0, 32.0)
    logit_multiplier = jax.random.uniform(latter_seed, (), jnp.float32, 10.0, 30.0)
    return jnp.stack([pooling_steepness, logit_multiplier])


def plant(result, key, smallest, high):
    spot = [jax.random.randint(jax.random.fold_in(key, axis), (), 0, length) for axis, length in enumerate(result.shape)]
    widest = result.shape.index(max(result.shape))
    next_to = spot[:widest] + [(spot[widest] + 1) % result.shape[widest]] + spot[widest + 1:]
    return result.at[tuple(spot)].set(smallest).at[tuple(next_to)].set(high)


def steps_of(stream_key, shape, cuts, smallest, largest):
    gain, own = 1.0, jax.random.fold_in(stream_key, 6)
    for axis_at, parts in cuts:
        heights = jnp.exp(jax.random.uniform(jax.random.fold_in(own, axis_at), (parts,), jnp.float32, smallest / len(cuts), largest / len(cuts)))
        gain = gain * jnp.repeat(heights, shape[axis_at] // parts).reshape([-1 if axis == axis_at else 1 for axis in range(len(shape))])
    return gain


def scatter_about(rng, shape, deviation, bound, cuts=(), kind=jnp.bfloat16):
    entries = deviation * jax.random.normal(rng, shape, jnp.float32)
    if cuts:
        entries = entries * steps_of(rng, shape, cuts, -0.22, 0.18)
    return jnp.clip(entries, -bound, bound).astype(kind)


def setup_inputs(seed: int = 0) -> dict:
    streams_of = jax.random.split(jax.random.key(seed), 8)
    return {
        "latent_states": draw_latent_states(jax.random.fold_in(streams_of[7], 71), 0),
        "rescale_factor": jnp.clip(1.0 + 0.15 * jax.random.normal(streams_of[1], (D,), jnp.float32), 0.25, 1.75),
        "embedding_matrix": scatter_about(streams_of[2], (D, E), D ** -0.5, 0.125, ((0, 4),)),
        "request_span": plant(jax.random.randint(streams_of[3], (MICRO, PAIRS_ALL), QLEN // 4, QLEN + 1), jax.random.fold_in(streams_of[3], 1), QLEN // 4, QLEN).astype(jnp.int32),
        "passage_span": plant(jax.random.randint(streams_of[4], (MICRO, PAIRS_ALL), QLEN, DLEN + 1), jax.random.fold_in(streams_of[4], 1), QLEN, DLEN).astype(jnp.int32),
        "matching_pair": jax.vmap(lambda own: jax.random.permutation(own, PAIRS_ALL))(jax.random.split(streams_of[5], MICRO)).reshape((MICRO, PAIRS_ALL)).astype(jnp.int32),
        "steepness_pair": draw_steepness_pair(jax.random.fold_in(streams_of[7], 71), 0),
    }


EPSILON = 1e-06
OBJECTIVE_FACTOR = 1024.0
MASKED = -1e+30

def head_forward(token_rows, rescale_factor, embedding_matrix):
    values = token_rows.astype(jnp.float32)
    inverse_rms = lax.rsqrt(lax.optimization_barrier(jnp.mean(values * values, axis=-1, keepdims=True)) + EPSILON)
    normed = (values * inverse_rms * rescale_factor).astype(jnp.bfloat16)
    projected = jnp.dot(normed, embedding_matrix, preferred_element_type=jnp.float32)
    inverse_length = lax.rsqrt(lax.optimization_barrier(jnp.sum(projected * projected, axis=-1, keepdims=True)) + EPSILON)
    vectors = (projected * inverse_length).astype(jnp.bfloat16)
    return (vectors, projected, inverse_length, inverse_rms)

def head_backward(token_rows, rescale_factor, embedding_matrix, projected, inverse_length, inverse_rms, grad_vectors):
    unit = projected * inverse_length
    along = lax.optimization_barrier(jnp.sum(unit * grad_vectors, axis=-1, keepdims=True))
    grad_projected = (inverse_length * (grad_vectors - unit * along)).astype(jnp.bfloat16)
    grad_normed = lax.dot_general(grad_projected, embedding_matrix, (((1,), (1,)), ((), ())), preferred_element_type=jnp.float32)
    values = token_rows.astype(jnp.float32)
    weighted = grad_normed * rescale_factor
    mean_term = lax.optimization_barrier(jnp.mean(values * weighted, axis=-1, keepdims=True))
    grad_rows = inverse_rms * weighted - values * (inverse_rms * inverse_rms * inverse_rms) * mean_term
    return grad_rows.astype(jnp.bfloat16)

def pool_tokens(similarity, pooling_steepness, live):
    scaled = jnp.where(live[None], pooling_steepness * similarity, MASKED)
    highest = lax.optimization_barrier(jnp.max(scaled, axis=2, keepdims=True))
    exponent = jnp.exp(scaled - highest)
    totals = lax.optimization_barrier(jnp.sum(exponent, axis=2, keepdims=True))
    smooth = (highest[:, :, 0] + jnp.log(totals[:, :, 0])) / pooling_steepness
    return (smooth, exponent / totals)

def versus_term(relevance_matrix, matching_pair, logit_multiplier):
    unnormalized_odds = logit_multiplier * relevance_matrix
    highest = lax.optimization_barrier(jnp.max(unnormalized_odds, axis=1, keepdims=True))
    log_total = highest[:, 0] + jnp.log(lax.optimization_barrier(jnp.sum(jnp.exp(unnormalized_odds - highest), axis=1)))
    columns = jnp.arange(relevance_matrix.shape[1], dtype=jnp.int32)
    correct_label = (columns[None, :] == matching_pair[:, None]).astype(jnp.float32)
    objective_value = log_total - lax.optimization_barrier(jnp.sum(unnormalized_odds * correct_label, axis=1))
    probability_share = jnp.exp(unnormalized_odds - log_total[:, None])
    score_slope = OBJECTIVE_FACTOR * logit_multiplier * (probability_share - correct_label)
    return (objective_value, score_slope)

def query_weights(request_span, count):
    places = jnp.arange(count, dtype=jnp.int32)
    ones = jnp.where(places[None, :] < request_span[:, None], 1.0, 0.0).astype(jnp.float32)
    return ones / request_span[:, None].astype(jnp.float32)

def live_tokens(passage_span, count):
    places = jnp.arange(count, dtype=jnp.int32)
    return places[None, :] < passage_span[:, None]

def single_micro_group(piece_tile, request_spans, passage_spans, selected_entry, rescale_factor, embedding_matrix, pooling_steepness, logit_multiplier):
    pairs, length, width = piece_tile.shape
    flat_rows = piece_tile.reshape(pairs * length, width)
    vectors, projected, inverse_length, inverse_rms = head_forward(flat_rows, rescale_factor, embedding_matrix)
    vectors = vectors.reshape(pairs, length, -1)
    features = vectors.shape[2]
    queries = vectors[:, :QLEN]
    doc_flat = vectors[:, QLEN:].reshape(pairs * DLEN, features)
    live = live_tokens(passage_spans, DLEN)
    weights = query_weights(request_spans, QLEN)

    def similarity_of(index):
        query = lax.dynamic_index_in_dim(queries, index, 0, keepdims=False)
        inner_product = lax.dot_general(query, doc_flat, (((1,), (1,)), ((), ())), preferred_element_type=jnp.float32)
        return (inner_product.reshape(QLEN, pairs, DLEN), query)

    def forward_pass(index):
        similarity, _ = similarity_of(index)
        smooth, _ = pool_tokens(similarity, pooling_steepness, live)
        row_weight = lax.dynamic_index_in_dim(weights, index, 0, keepdims=False)
        return lax.optimization_barrier(jnp.sum(smooth * row_weight[:, None], axis=0))
    indices = jnp.arange(pairs, dtype=jnp.int32)
    relevance_matrix = lax.map(forward_pass, indices)
    objective_value, score_slope = versus_term(relevance_matrix, selected_entry, logit_multiplier)

    def backward(carry, index):
        similarity, query = similarity_of(index)
        _, token_weight = pool_tokens(similarity, pooling_steepness, live)
        row_weight = lax.dynamic_index_in_dim(weights, index, 0, keepdims=False)
        grad_row = lax.dynamic_index_in_dim(score_slope, index, 0, keepdims=False)
        coefficient = row_weight[:, None] * grad_row[None, :]
        similarity_gradient = (coefficient[:, :, None] * token_weight).astype(jnp.bfloat16).reshape(QLEN, pairs * DLEN)
        grad_query = jnp.dot(similarity_gradient, doc_flat, preferred_element_type=jnp.float32)
        carry = carry + lax.dot_general(similarity_gradient, query, (((0,), (0,)), ((), ())), preferred_element_type=jnp.float32)
        return (carry, grad_query)
    grad_docs, grad_queries = lax.scan(backward, jnp.zeros((pairs * DLEN, features), jnp.float32), indices)
    grad_vectors = jnp.concatenate([grad_queries.reshape(pairs, QLEN, features), grad_docs.reshape(pairs, DLEN, features)], axis=1)
    grad_rows = head_backward(flat_rows, rescale_factor, embedding_matrix, projected, inverse_length, inverse_rms, grad_vectors.reshape(pairs * length, features))
    return (grad_rows.reshape(pairs, length, width), objective_value)

def reference(latent_states, rescale_factor, embedding_matrix, request_span, passage_span, matching_pair, steepness_pair):
    pooling_steepness = steepness_pair[0]
    logit_multiplier = steepness_pair[1]

    def per_batch(inputs):
        piece_tile, request_spans, passage_spans, selected_entry = inputs
        return single_micro_group(piece_tile, request_spans, passage_spans, selected_entry, rescale_factor, embedding_matrix, pooling_steepness, logit_multiplier)
    grad_hidden, losses = lax.map(per_batch, (latent_states, request_span, passage_span, matching_pair))
    return (grad_hidden, losses)
```

```python
import functools

import jax
import jax.numpy as jnp
from jax import lax
from jax.experimental import pallas as pl
from jax.experimental.pallas import tpu as pltpu
from jax.sharding import Mesh
from jax.sharding import PartitionSpec as P

QLEN = 32
DLEN = 64
SECTION = ("h", "k")
PLANE = ("x", "y")
DP = ("x", "y", "z")

EPSILON = 1e-06
OBJECTIVE_FACTOR = 1024.0
MASKED = -1e30

f32 = jnp.float32
bf16 = jnp.bfloat16


def vmem():
    return pl.BlockSpec(memory_space=pltpu.VMEM)


def smem():
    return pl.BlockSpec(memory_space=pltpu.SMEM)


def dot_nt(a, b):
    return lax.dot_general(a, b, (((1,), (1,)), ((), ())), preferred_element_type=f32)


def dot_tn(a, b):
    return lax.dot_general(a, b, (((0,), (0,)), ((), ())), preferred_element_type=f32)


def section_index():
    return lax.axis_index("h"), lax.axis_index("k")


def head_forward_kernel(x_ref, gain_ref, own_ref, core_ref, far_ref, far_core_ref,
                        q_ref, d_ref, proj_ref, emb_ref):
    depth = own_ref.shape[0]

    @pl.when(pl.program_id(0) == 0)
    def _():
        h, k = section_index()
        for ref, section in (
            (own_ref, h * 2 + k),
            (core_ref, h * 2 + 1 - k),
            (far_ref, (1 - h) * 2 + k),
            (far_core_ref, (1 - h) * 2 + 1 - k),
        ):
            emb_ref[pl.ds(pl.multiple_of(section * depth, depth), depth), :] = ref[...]

    values = x_ref[0].astype(f32)
    inverse_rms = lax.rsqrt(jnp.mean(values * values, axis=-1, keepdims=True) + EPSILON)
    normed = (values * inverse_rms * gain_ref[...]).astype(bf16)
    projected = jnp.dot(normed, emb_ref[...], preferred_element_type=f32)
    inverse_length = lax.rsqrt(jnp.sum(projected * projected, axis=-1, keepdims=True) + EPSILON)
    vectors = (projected * inverse_length).astype(bf16)
    q_ref[...] = vectors[:QLEN]
    d_ref[...] = vectors[QLEN:]
    proj_ref[0] = projected


def head_forward(x, gain, slices):
    pairs, length, width = x.shape
    depth, features = slices[0].shape
    whole = lambda *shape: pl.BlockSpec(shape, lambda i: (0,) * len(shape))
    return pl.pallas_call(
        head_forward_kernel,
        grid=(pairs,),
        in_specs=[
            pl.BlockSpec((1, length, width), lambda i: (i, 0, 0)),
            whole(1, width),
            *[whole(depth, features) for _ in slices],
        ],
        out_specs=[
            pl.BlockSpec((QLEN, features), lambda i: (i, 0)),
            pl.BlockSpec((DLEN, features), lambda i: (i, 0)),
            pl.BlockSpec((1, length, features), lambda i: (i, 0, 0)),
            whole(width, features),
        ],
        out_shape=[
            jax.ShapeDtypeStruct((pairs * QLEN, features), bf16),
            jax.ShapeDtypeStruct((pairs * DLEN, features), bf16),
            jax.ShapeDtypeStruct((pairs, length, features), f32),
            jax.ShapeDtypeStruct((width, features), bf16),
        ],
        name="head_forward",
    )(x, gain, *slices)


def ring_slot(shift, z, ring):
    return lax.rem(z + shift + ring, ring)


def place_queries(refs, all_ref):
    ring = len(refs)
    z = lax.axis_index("z")
    rows = refs[0].shape[0]
    for shift, ref in enumerate(refs):
        slot = ring_slot(-shift, z, ring)
        all_ref[pl.ds(pl.multiple_of(slot * rows, rows), rows), :] = ref[...]


def query_lanes(spans_ref, micro, first, count):
    lanes = count * QLEN
    lane = lax.broadcasted_iota(jnp.int32, (1, lanes), 1)
    owner = lax.div(lane, QLEN)
    filled = jnp.zeros((1, lanes), jnp.int32)
    for b in range(count):
        filled = jnp.where(owner == b, spans_ref[micro, first + b], filled)
    return filled


def micro_index():
    h, k = section_index()
    return h * 2 + k


def first_row():
    ring = lax.axis_size("z")
    return (lax.axis_index("x") * lax.axis_size("y") + lax.axis_index("y")) * ring


def document_pair(c, pairs):
    ring = lax.axis_size("z")
    return (lax.div(c, pairs) * ring + lax.axis_index("z")) * pairs + lax.rem(c, pairs)


def scores_kernel(pairs, group, request_ref, passage_ref, match_ref, steep_ref,
                  docs_ref, q0, q1, q2, q3,
                  q_all, level_ref, logits_ref, stats_ref, sim_a, sim_b):
    micro = micro_index()
    beta = steep_ref[0]
    mult = steep_ref[1]
    place_queries((q0, q1, q2, q3), q_all)
    rows = group * DLEN
    blocks = docs_ref.shape[0] // rows
    lanes = q_all.shape[0]
    token = lax.broadcasted_iota(jnp.int32, (DLEN, 1), 0)

    def similarity(block, ref):
        start = pl.multiple_of(block * rows, rows)
        ref[...] = dot_nt(docs_ref[pl.ds(start, rows), :], q_all[...])

    def pool(block, ref):
        levels = []
        for n in range(group):
            c = block * group + n
            span = passage_ref[micro, document_pair(c, pairs)]
            scaled = jnp.where(token < span, beta * ref[n * DLEN:(n + 1) * DLEN, :], MASKED)
            highest = jnp.max(scaled, axis=0, keepdims=True)
            total = jnp.sum(jnp.exp(scaled - highest), axis=0, keepdims=True)
            levels.append(highest + jnp.log(total))
        level_ref[pl.ds(pl.multiple_of(block * group, group), group), :] = jnp.concatenate(levels, axis=0)

    similarity(0, sim_a)

    def step(i, carry):
        similarity(2 * i + 1, sim_b)
        pool(2 * i, sim_a)
        similarity(jnp.minimum(2 * i + 2, blocks - 1), sim_a)
        pool(2 * i + 1, sim_b)
        return carry

    lax.fori_loop(0, blocks // 2, step, 0)

    count = lanes // QLEN
    first = first_row() * pairs
    span = query_lanes(request_ref, micro, first, count)
    match = query_lanes(match_ref, micro, first, count)
    lane = lax.broadcasted_iota(jnp.int32, (1, lanes), 1)
    weight = jnp.where(lax.rem(lane, QLEN) < span, 1.0, 0.0).astype(f32) / span.astype(f32)
    same = (
        lax.div(lax.broadcasted_iota(jnp.int32, (lanes, lanes), 0), QLEN)
        == lax.div(lax.broadcasted_iota(jnp.int32, (lanes, lanes), 1), QLEN)
    ).astype(f32)
    smooth = level_ref[...] / beta
    scores = jnp.dot(smooth * weight, same, preferred_element_type=f32, precision=lax.Precision.HIGHEST)
    logits = mult * scores
    logits_ref[...] = logits
    docs = logits.shape[0]
    column = document_pair(lax.broadcasted_iota(jnp.int32, (docs, 1), 0), pairs)
    highest = jnp.max(logits, axis=0, keepdims=True)
    local = highest + jnp.log(jnp.sum(jnp.exp(logits - highest), axis=0, keepdims=True))
    positive = jnp.sum(jnp.where(column == match, logits, 0.0), axis=0, keepdims=True)
    stats_ref[...] = jnp.concatenate([local, positive], axis=0)


def scores_forward(spans, steep, docs, queries, pairs):
    rows, features = queries[0].shape
    lanes = rows * len(queries)
    count = docs.shape[0] // DLEN
    group = 8
    return pl.pallas_call(
        functools.partial(scores_kernel, pairs, group),
        in_specs=[smem()] * 4 + [vmem()] * 5,
        out_specs=[vmem()] * 4,
        out_shape=[
            jax.ShapeDtypeStruct((lanes, features), bf16),
            jax.ShapeDtypeStruct((count, lanes), f32),
            jax.ShapeDtypeStruct((count, lanes), f32),
            jax.ShapeDtypeStruct((2, lanes), f32),
        ],
        scratch_shapes=[pltpu.VMEM((group * DLEN, lanes), f32)] * 2,
        name="scores_forward",
    )(*spans, steep, docs, *queries)


def grads_kernel(pairs, group, request_ref, passage_ref, match_ref, steep_ref,
                 docs_ref, q_all, level_ref, logits_ref, s0, s1, s2, s3,
                 gd_ref, gq0, gq1, gq2, gq3, loss_ref,
                 sim_a, sim_b, grad_a, grad_b, coef_ref, acc_ref, turned_ref):
    micro = micro_index()
    beta = steep_ref[0]
    mult = steep_ref[1]
    rows = group * DLEN
    blocks = docs_ref.shape[0] // rows
    lanes = q_all.shape[0]
    count = lanes // QLEN
    ring = lax.axis_size("z")
    z = lax.axis_index("z")
    first = first_row() * pairs
    span = query_lanes(request_ref, micro, first, count)
    match = query_lanes(match_ref, micro, first, count)
    lane = lax.broadcasted_iota(jnp.int32, (1, lanes), 1)
    weight = jnp.where(lax.rem(lane, QLEN) < span, 1.0, 0.0).astype(f32) / span.astype(f32)

    stats = [s0[...], s1[...], s2[...], s3[...]]
    locals_ = [s[0:1] for s in stats]
    highest = functools.reduce(jnp.maximum, locals_)
    total = sum(jnp.exp(l - highest) for l in locals_)
    log_total = highest + jnp.log(total)
    positive = sum(s[1:2] for s in stats)
    loss_ref[...] = log_total - positive

    docs = logits_ref.shape[0]
    column = document_pair(lax.broadcasted_iota(jnp.int32, (docs, 1), 0), pairs)
    share = jnp.exp(logits_ref[...] - log_total) - jnp.where(column == match, 1.0, 0.0)
    coef_ref[...] = weight * (OBJECTIVE_FACTOR * mult * share)

    token = lax.broadcasted_iota(jnp.int32, (DLEN, 1), 0)
    acc_ref[...] = jnp.zeros_like(acc_ref)

    def similarity(block, ref):
        start = pl.multiple_of(block * rows, rows)
        ref[...] = dot_nt(docs_ref[pl.ds(start, rows), :], q_all[...])

    def weigh(block, ref, grad):
        base = pl.multiple_of(block * group, group)
        level = level_ref[pl.ds(base, group), :]
        coef = coef_ref[pl.ds(base, group), :]
        for n in range(group):
            c = block * group + n
            live = passage_ref[micro, document_pair(c, pairs)]
            at = slice(n * DLEN, (n + 1) * DLEN)
            scaled = jnp.where(token < live, beta * ref[at, :], MASKED)
            share = jnp.exp(scaled - level[n:n + 1])
            grad[at, :] = (coef[n:n + 1] * share).astype(bf16)

    def reduce(block, grad):
        start = pl.multiple_of(block * rows, rows)
        gd_ref[pl.ds(start, rows), :] = jnp.dot(
            grad[...], q_all[...], preferred_element_type=f32
        ).astype(gd_ref.dtype)
        acc_ref[...] += dot_tn(docs_ref[pl.ds(start, rows), :], grad[...])

    similarity(0, sim_a)

    def step(i, carry):
        similarity(2 * i + 1, sim_b)
        weigh(2 * i, sim_a, grad_a)
        similarity(jnp.minimum(2 * i + 2, blocks - 1), sim_a)
        reduce(2 * i, grad_a)
        weigh(2 * i + 1, sim_b, grad_b)
        reduce(2 * i + 1, grad_b)
        return carry

    lax.fori_loop(0, blocks // 2, step, 0)
    turned_ref[...] = acc_ref[...].T
    own = lanes // ring
    for shift, ref in enumerate((gq0, gq1, gq2, gq3)):
        slot = ring_slot(shift, z, ring)
        ref[...] = turned_ref[pl.ds(pl.multiple_of(slot * own, own), own), :]


def scores_backward(spans, steep, docs, q_all, level, logits, stats, pairs):
    lanes, features = q_all.shape
    rows = lanes // len(stats)
    count = level.shape[0]
    group = 8
    return pl.pallas_call(
        functools.partial(grads_kernel, pairs, group),
        in_specs=[smem()] * 4 + [vmem()] * 8,
        out_specs=[vmem()] * 6,
        out_shape=[
            jax.ShapeDtypeStruct(docs.shape, bf16),
            *[jax.ShapeDtypeStruct((rows, features), f32)] * 4,
            jax.ShapeDtypeStruct((1, lanes), f32),
        ],
        scratch_shapes=[pltpu.VMEM((group * DLEN, lanes), f32)] * 2
        + [pltpu.VMEM((group * DLEN, lanes), bf16)] * 2
        + [
            pltpu.VMEM((count, lanes), f32),
            pltpu.VMEM((features, lanes), f32),
            pltpu.VMEM((lanes, features), f32),
        ],
        name="scores_backward",
    )(*spans, steep, docs, q_all, level, logits, *stats)


def head_backward_kernel(x_ref, gain_ref, emb_ref, proj_ref, gd_ref, g0, g1, g2, g3, out_ref):
    grad_query = g0[...] + g1[...] + g2[...] + g3[...]
    grad_docs = jnp.sum(gd_ref[...].astype(f32), axis=0)
    grad_vectors = jnp.concatenate([grad_query, grad_docs], axis=0)
    projected = proj_ref[0]
    inverse_length = lax.rsqrt(jnp.sum(projected * projected, axis=-1, keepdims=True) + EPSILON)
    unit = projected * inverse_length
    along = jnp.sum(unit * grad_vectors, axis=-1, keepdims=True)
    grad_projected = (inverse_length * (grad_vectors - unit * along)).astype(bf16)
    values = x_ref[0].astype(f32)
    inverse_rms = lax.rsqrt(jnp.mean(values * values, axis=-1, keepdims=True) + EPSILON)
    weighted = dot_nt(grad_projected, emb_ref[...]) * gain_ref[...]
    mean_term = jnp.mean(values * weighted, axis=-1, keepdims=True)
    out_ref[0] = (
        inverse_rms * weighted - values * (inverse_rms * inverse_rms * inverse_rms) * mean_term
    ).astype(bf16)


def head_backward(x, gain, emb, projected, grad_docs, grad_queries):
    pairs, length, width = x.shape
    features = emb.shape[1]
    senders = grad_docs.shape[0]
    whole = lambda *shape: pl.BlockSpec(shape, lambda i: (0,) * len(shape))
    return pl.pallas_call(
        head_backward_kernel,
        grid=(pairs,),
        in_specs=[
            pl.BlockSpec((1, length, width), lambda i: (i, 0, 0)),
            whole(1, width),
            whole(width, features),
            pl.BlockSpec((1, length, features), lambda i: (i, 0, 0)),
            pl.BlockSpec((senders, DLEN, features), lambda i: (0, i, 0)),
            *[pl.BlockSpec((QLEN, features), lambda i: (i, 0))] * 4,
        ],
        out_specs=pl.BlockSpec((1, length, width), lambda i: (i, 0, 0)),
        out_shape=jax.ShapeDtypeStruct(x.shape, bf16),
        name="head_backward",
    )(x, gain, emb, projected, grad_docs, *grad_queries)


def all_slices(own):
    swap = [(0, 1), (1, 0)]
    ring = lax.axis_size("z")
    mirror = [
        (h * ring + z, (1 - h) * ring + ring - 1 - z) for h in range(2) for z in range(ring)
    ]
    far = lax.ppermute(own, ("h", "z"), mirror)
    core = lax.ppermute(own, "k", swap)
    far_core = lax.ppermute(far, "k", swap)
    return own, core, far, far_core


def turned(array, shift):
    ring = lax.axis_size("z")
    return lax.ppermute(array, "z", [(i, (i + shift) % ring) for i in range(ring)])


def local(x, gain, embedding, request_span, passage_span, matching_pair, steepness):
    x = x[0]
    pairs = x.shape[0]
    ring = lax.axis_size("z")
    gain = gain[None]
    spans = (request_span, passage_span, matching_pair)
    q, d, projected, emb = head_forward(x, gain, all_slices(embedding))
    queries = [q] + [turned(q, s) for s in range(1, ring)]
    plane = lax.axis_size(PLANE)
    copies = jnp.broadcast_to(d, (plane, *d.shape))
    docs = lax.all_to_all(copies, PLANE, split_axis=0, concat_axis=0, tiled=True)
    docs = docs.reshape(plane * d.shape[0], d.shape[1])
    q_all, level, logits, stats = scores_forward(spans, steepness, docs, queries, pairs)
    stats = [stats] + [turned(stats, s) for s in range(1, ring)]
    gd, g0, g1, g2, g3, loss = scores_backward(
        spans, steepness, docs, q_all, level, logits, stats, pairs
    )
    grad_docs = lax.all_to_all(
        gd.reshape(plane, *d.shape), PLANE, split_axis=0, concat_axis=0, tiled=True
    )
    grad_queries = [g0] + [turned(g, s) for s, g in ((1, g1), (2, g2), (3, g3))]
    grad_x = head_backward(x, gain, emb, projected, grad_docs, grad_queries)
    own = lax.dynamic_slice_in_dim(
        loss.reshape(ring, pairs, QLEN)[:, :, 0], lax.axis_index("z"), 1, 0
    )
    return grad_x[None], own


def solution(mesh):
    side = round(mesh.shape["dp"] ** (1 / 3))
    finer = Mesh(mesh.devices.reshape(2, 2, side, side, side), ("h", "k", "x", "y", "z"))
    rows = P(SECTION, DP, None, None)
    return jax.shard_map(
        local,
        mesh=finer,
        in_specs=(rows, P(), P(SECTION, None), P(), P(), P(), P()),
        out_specs=(rows, P(SECTION, DP)),
        check_vma=False,
    )
```

```python
import functools

import jax
import jax.numpy as jnp
from jax import lax
from jax.experimental import pallas as pl
from jax.experimental.pallas import tpu as pltpu
from jax.sharding import Mesh
from jax.sharding import PartitionSpec as P

QLEN = 32
DLEN = 64
UNROLL_F = True
UNROLL_B = True
GROUP_F = 8
GROUP_B = 8
DLEN_LEAST = 32
SECTION = ("h", "k")
PLANE = ("x", "y")
DP = ("x", "y", "z")

EPSILON = 1e-06
OBJECTIVE_FACTOR = 1024.0
MASKED = -1e30

LOG2_E = 1.4426950408889634
LN_2 = 0.6931471805599453

f32 = jnp.float32
bf16 = jnp.bfloat16


def grant(mib):
    return pltpu.CompilerParams(vmem_limit_bytes=mib * 1024 * 1024)


def vmem():
    return pl.BlockSpec(memory_space=pltpu.VMEM)


def hbm():
    return pl.BlockSpec(memory_space=pltpu.HBM)


def smem():
    return pl.BlockSpec(memory_space=pltpu.SMEM)


def rows_at(block, rows):
    start = block * rows
    return pl.ds(start if isinstance(start, int) else pl.multiple_of(start, rows), rows)


def dot_nt(a, b):
    return lax.dot_general(a, b, (((1,), (1,)), ((), ())), preferred_element_type=f32)


def dot_tn(a, b):
    return lax.dot_general(a, b, (((0,), (0,)), ((), ())), preferred_element_type=f32)


def in_turn(blocks, unroll, first, one):
    first(0, 0)

    def step(i, carry):
        first(2 * i + 1, 1)
        one(2 * i, 0)
        first(jnp.minimum(2 * i + 2, blocks - 1), 0)
        one(2 * i + 1, 1)
        return carry

    if unroll:
        for block in range(blocks):
            if block + 1 < blocks:
                first(block + 1, (block + 1) % 2)
            one(block, block % 2)
    else:
        lax.fori_loop(0, blocks // 2, step, 0)


def section_index():
    return lax.axis_index("h"), lax.axis_index("k")


def normalize_kernel(x_ref, gain_ref, normed_ref):
    values = x_ref[0].astype(f32)
    inverse_rms = lax.rsqrt(jnp.mean(values * values, axis=-1, keepdims=True) + EPSILON)
    normed_ref[0] = (values * inverse_rms * gain_ref[...]).astype(bf16)


def normalize(x, gain):
    pairs, length, width = x.shape
    rows = pl.BlockSpec((1, length, width), lambda i: (i, 0, 0))
    return pl.pallas_call(
        normalize_kernel,
        grid=(pairs,),
        in_specs=[rows, pl.BlockSpec((1, width), lambda i: (0, 0))],
        out_specs=rows,
        out_shape=jax.ShapeDtypeStruct(x.shape, bf16),
        compiler_params=grant(6),
        name="normalize",
    )(x, gain)


def project_kernel(normed_ref, own_ref, core_ref, far_ref, far_core_ref,
                   q_ref, copies_ref, proj_ref, emb_ref, d_ref, sems):
    depth = own_ref.shape[0]
    h, k = section_index()
    for ref, section in (
        (own_ref, h * 2 + k),
        (core_ref, h * 2 + 1 - k),
        (far_ref, (1 - h) * 2 + k),
        (far_core_ref, (1 - h) * 2 + 1 - k),
    ):
        emb_ref[pl.ds(pl.multiple_of(section * depth, depth), depth), :] = ref[...]
    pairs, _, _ = normed_ref.shape
    for p in range(pairs):
        projected = jnp.dot(normed_ref[p], emb_ref[...], preferred_element_type=f32)
        inverse_length = lax.rsqrt(
            jnp.sum(projected * projected, axis=-1, keepdims=True) + EPSILON
        )
        vectors = (projected * inverse_length).astype(bf16)
        q_ref[p * QLEN:(p + 1) * QLEN] = vectors[:QLEN]
        d_ref[p * DLEN:(p + 1) * DLEN] = vectors[QLEN:]
        proj_ref[p] = projected
    copies = [
        pltpu.make_async_copy(d_ref, copies_ref.at[n], sems.at[n])
        for n in range(copies_ref.shape[0])
    ]
    for copy in copies:
        copy.start()
    for copy in copies:
        copy.wait()


def project(normed, slices, readers):
    pairs, length, width = normed.shape
    _, features = slices[0].shape
    return pl.pallas_call(
        project_kernel,
        in_specs=[vmem()] * 5,
        out_specs=[vmem(), hbm(), vmem(), vmem()],
        out_shape=[
            jax.ShapeDtypeStruct((pairs * QLEN, features), bf16),
            pltpu.HBM((readers, pairs * DLEN, features), bf16),
            jax.ShapeDtypeStruct((pairs, length, features), f32),
            jax.ShapeDtypeStruct((width, features), bf16),
        ],
        scratch_shapes=[
            pltpu.VMEM((pairs * DLEN, features), bf16),
            pltpu.SemaphoreType.DMA((readers,)),
        ],
        compiler_params=grant(6),
        name="project",
    )(normed, *slices)


def ring_slot(shift, z, ring):
    return lax.rem(z + shift + ring, ring)


def place_queries(refs, all_ref):
    ring = len(refs)
    z = lax.axis_index("z")
    rows = refs[0].shape[0]
    for shift, ref in enumerate(refs):
        slot = ring_slot(-shift, z, ring)
        all_ref[pl.ds(pl.multiple_of(slot * rows, rows), rows), :] = ref[...]


def query_lanes(spans_ref, micro, first, count):
    lanes = count * QLEN
    lane = lax.broadcasted_iota(jnp.int32, (1, lanes), 1)
    owner = lax.div(lane, QLEN)
    filled = jnp.zeros((1, lanes), jnp.int32)
    for b in range(count):
        filled = jnp.where(owner == b, spans_ref[micro, first + b], filled)
    return filled


def micro_index():
    h, k = section_index()
    return h * 2 + k


def first_row():
    ring = lax.axis_size("z")
    return (lax.axis_index("x") * lax.axis_size("y") + lax.axis_index("y")) * ring


def document_pair(c, pairs):
    ring = lax.axis_size("z")
    return (lax.div(c, pairs) * ring + lax.axis_index("z")) * pairs + lax.rem(c, pairs)


def spread_sums(terms):
    _, lanes = terms.shape
    wide = 128
    same = (
        lax.div(lax.broadcasted_iota(jnp.int32, (wide, wide), 0), QLEN)
        == lax.div(lax.broadcasted_iota(jnp.int32, (wide, wide), 1), QLEN)
    ).astype(bf16)
    high = terms.astype(bf16)
    rest = terms - high.astype(f32)
    middle = rest.astype(bf16)
    low = (rest - middle.astype(f32)).astype(bf16)
    sums = []
    for at in range(0, lanes, wide):
        parts = [
            jnp.dot(part[:, at:at + wide], same, preferred_element_type=f32)
            for part in (low, middle, high)
        ]
        sums.append(parts[0] + parts[1] + parts[2])
    return jnp.concatenate(sums, axis=1)


def scores_kernel(pairs, group, request_ref, passage_ref, match_ref, steep_ref,
                  docs_ref, q0, q1, q2, q3,
                  q_all, level_ref, logits_ref, stats_ref, *sims):
    micro = micro_index()
    beta2 = steep_ref[0] * LOG2_E
    mult = steep_ref[1]
    place_queries((q0, q1, q2, q3), q_all)
    rows = group * DLEN
    blocks = docs_ref.shape[0] // rows
    lanes = q_all.shape[0]
    token = lax.broadcasted_iota(jnp.int32, (DLEN - DLEN_LEAST, 1), 0) + DLEN_LEAST

    def similarity(block, slot):
        sims[slot][...] = dot_nt(docs_ref[rows_at(block, rows), :], q_all[...])

    def pool(block, slot):
        ref = sims[slot]
        levels = []
        for n in range(group):
            c = block * group + n
            span = passage_ref[micro, document_pair(c, pairs)]
            at = n * DLEN
            early = ref[at:at + DLEN_LEAST, :]
            late = jnp.where(token < span, ref[at + DLEN_LEAST:at + DLEN, :], MASKED)
            highest = jnp.max(jnp.maximum(early, late), axis=0, keepdims=True)
            total = jnp.sum(
                jnp.exp2(beta2 * (early - highest)) + jnp.exp2(beta2 * (late - highest)),
                axis=0,
                keepdims=True,
            )
            levels.append(beta2 * highest + jnp.log2(total))
        level_ref[rows_at(block, group), :] = jnp.concatenate(levels, axis=0)

    in_turn(blocks, UNROLL_F, similarity, pool)

    count = lanes // QLEN
    first = first_row() * pairs
    span = query_lanes(request_ref, micro, first, count)
    match = query_lanes(match_ref, micro, first, count)
    lane = lax.broadcasted_iota(jnp.int32, (1, lanes), 1)
    weight = jnp.where(lax.rem(lane, QLEN) < span, 1.0, 0.0).astype(f32) / span.astype(f32)
    smooth = level_ref[...] * (LN_2 / steep_ref[0])
    logits = mult * spread_sums(smooth * weight)
    logits_ref[...] = logits
    docs = logits.shape[0]
    column = document_pair(lax.broadcasted_iota(jnp.int32, (docs, 1), 0), pairs)
    highest = jnp.max(logits, axis=0, keepdims=True)
    local = highest + jnp.log(jnp.sum(jnp.exp(logits - highest), axis=0, keepdims=True))
    positive = jnp.sum(jnp.where(column == match, logits, 0.0), axis=0, keepdims=True)
    stats_ref[...] = jnp.concatenate([local, positive], axis=0)


def scores_forward(spans, steep, docs, queries, pairs):
    rows, features = queries[0].shape
    lanes = rows * len(queries)
    count = docs.shape[0] // DLEN
    group = GROUP_F
    return pl.pallas_call(
        functools.partial(scores_kernel, pairs, group),
        in_specs=[smem()] * 4 + [vmem()] * 5,
        out_specs=[vmem()] * 4,
        out_shape=[
            jax.ShapeDtypeStruct((lanes, features), bf16),
            jax.ShapeDtypeStruct((count, lanes), f32),
            jax.ShapeDtypeStruct((count, lanes), f32),
            jax.ShapeDtypeStruct((2, lanes), f32),
        ],
        scratch_shapes=[pltpu.VMEM((group * DLEN, lanes), f32)] * 2,
        compiler_params=grant(10),
        name="scores_forward",
    )(*spans, steep, docs, *queries)


def slopes_kernel(pairs, group, request_ref, passage_ref, match_ref, steep_ref,
                  docs_ref, q_all, level_ref, logits_ref, s0, s1, s2, s3,
                  gd_ref, gq0, gq1, gq2, gq3, loss_ref,
                 sim_a, sim_b, coef_ref, gd_vmem, acc_ref, turned_ref, sem, sems):
    micro = micro_index()
    beta2 = steep_ref[0] * LOG2_E
    mult = steep_ref[1]
    rows = group * DLEN
    blocks = docs_ref.shape[0] // rows
    lanes = q_all.shape[0]
    count = lanes // QLEN
    first = first_row() * pairs
    span = query_lanes(request_ref, micro, first, count)
    match = query_lanes(match_ref, micro, first, count)
    lane = lax.broadcasted_iota(jnp.int32, (1, lanes), 1)
    weight = jnp.where(lax.rem(lane, QLEN) < span, 1.0, 0.0).astype(f32) / span.astype(f32)

    stats = [s0[...], s1[...], s2[...], s3[...]]
    locals_ = [s[0:1] for s in stats]
    highest = functools.reduce(jnp.maximum, locals_)
    total = sum(jnp.exp(l - highest) for l in locals_)
    log_total = highest + jnp.log(total)
    positive = sum(s[1:2] for s in stats)
    loss_ref[...] = log_total - positive

    docs = logits_ref.shape[0]
    column = document_pair(lax.broadcasted_iota(jnp.int32, (docs, 1), 0), pairs)
    share = jnp.exp(logits_ref[...] - log_total) - jnp.where(column == match, 1.0, 0.0)
    coef_ref[...] = weight * (OBJECTIVE_FACTOR * mult * share)

    token = lax.broadcasted_iota(jnp.int32, (DLEN - DLEN_LEAST, 1), 0) + DLEN_LEAST
    sims = (sim_a, sim_b)

    def similarity(block, slot):
        sims[slot][...] = dot_nt(docs_ref[rows_at(block, rows), :], q_all[...])

    def weigh(block, slot):
        ref = sims[slot]
        level = level_ref[rows_at(block, group), :]
        coef = coef_ref[rows_at(block, group), :]
        parts = []
        for n in range(group):
            live = passage_ref[micro, document_pair(block * group + n, pairs)]
            at = n * DLEN
            share = jnp.exp2(beta2 * ref[at:at + DLEN_LEAST, :] - level[n:n + 1])
            parts.append((coef[n:n + 1] * share).astype(bf16))
            share = jnp.exp2(beta2 * ref[at + DLEN_LEAST:at + DLEN, :] - level[n:n + 1])
            parts.append(jnp.where(token < live, coef[n:n + 1] * share, 0.0).astype(bf16))
        grad = jnp.concatenate(parts, axis=0)
        gd_vmem[rows_at(block, rows), :] = jnp.dot(
            grad, q_all[...], preferred_element_type=f32
        ).astype(gd_ref.dtype)
        acc_ref[...] += dot_tn(docs_ref[rows_at(block, rows), :], grad)

    acc_ref[...] = jnp.zeros_like(acc_ref)
    in_turn(blocks, UNROLL_B, similarity, weigh)
    out = pltpu.make_async_copy(gd_vmem.reshape(gd_ref.shape), gd_ref, sem)
    out.start()
    parts = (gq0, gq1, gq2, gq3)
    own = lanes // len(parts)
    turned_ref[...] = acc_ref[...].T
    z = lax.axis_index("z")
    sends = [out]
    for shift, ref in enumerate(parts):
        at = rows_at(ring_slot(shift, z, len(parts)), own)
        sends.append(pltpu.make_async_copy(turned_ref.at[at], ref, sems.at[shift]))
        sends[-1].start()
    for send in sends:
        send.wait()


def slopes(spans, steep, docs, q_all, level, logits, stats, pairs, block_shape):
    lanes, features = q_all.shape
    count = level.shape[0]
    group = GROUP_B
    return pl.pallas_call(
        functools.partial(slopes_kernel, pairs, group),
        in_specs=[smem()] * 4 + [vmem()] * 8,
        out_specs=[hbm()] * (len(stats) + 1) + [vmem()],
        out_shape=[
            pltpu.HBM(block_shape, bf16),
            *[pltpu.HBM((lanes // len(stats), features), f32)] * len(stats),
            jax.ShapeDtypeStruct((1, lanes), f32),
        ],
        scratch_shapes=[
            pltpu.VMEM((group * DLEN, lanes), f32),
            pltpu.VMEM((group * DLEN, lanes), f32),
            pltpu.VMEM((count, lanes), f32),
            pltpu.VMEM(docs.shape, bf16),
            pltpu.VMEM((features, lanes), f32),
            pltpu.VMEM((lanes, features), f32),
            pltpu.SemaphoreType.DMA,
            pltpu.SemaphoreType.DMA((len(stats),)),
        ],
        compiler_params=grant(16),
        name="slopes",
    )(*spans, steep, docs, q_all, level, logits, *stats)


def head_backward_kernel(x_ref, gain_ref, emb_ref, proj_ref, gd_ref, g0, g1, g2, g3, out_ref,
                         out_vmem, sems):
    pairs = x_ref.shape[0]
    sends = []
    for p in range(pairs):
        at = slice(p * QLEN, (p + 1) * QLEN)
        grad_query = g0[at] + g1[at] + g2[at] + g3[at]
        grad_docs = jnp.sum(gd_ref[:, p * DLEN:(p + 1) * DLEN].astype(f32), axis=0)
        grad_vectors = jnp.concatenate([grad_query, grad_docs], axis=0)
        projected = proj_ref[p]
        inverse_length = lax.rsqrt(
            jnp.sum(projected * projected, axis=-1, keepdims=True) + EPSILON
        )
        unit = projected * inverse_length
        along = jnp.sum(unit * grad_vectors, axis=-1, keepdims=True)
        grad_projected = (inverse_length * (grad_vectors - unit * along)).astype(bf16)
        values = x_ref[p].astype(f32)
        inverse_rms = lax.rsqrt(jnp.mean(values * values, axis=-1, keepdims=True) + EPSILON)
        weighted = dot_nt(grad_projected, emb_ref[...]) * gain_ref[...]
        mean_term = jnp.mean(values * weighted, axis=-1, keepdims=True)
        out_vmem[p] = (
            inverse_rms * weighted
            - values * (inverse_rms * inverse_rms * inverse_rms) * mean_term
        ).astype(bf16)
        sends.append(pltpu.make_async_copy(out_vmem.at[p], out_ref.at[p], sems.at[p]))
        sends[-1].start()
    for send in sends:
        send.wait()


def head_backward(x, gain, emb, projected, grad_docs, grad_queries):
    pairs = x.shape[0]
    return pl.pallas_call(
        head_backward_kernel,
        in_specs=[vmem()] * 9,
        out_specs=hbm(),
        out_shape=jax.ShapeDtypeStruct(x.shape, bf16),
        scratch_shapes=[pltpu.VMEM(x.shape, bf16), pltpu.SemaphoreType.DMA((pairs,))],
        compiler_params=grant(10),
        name="head_backward",
    )(x, gain, emb, projected, grad_docs, *grad_queries)


def all_slices(own):
    swap = [(0, 1), (1, 0)]
    ring = lax.axis_size("z")
    mirror = [
        (h * ring + z, (1 - h) * ring + ring - 1 - z) for h in range(2) for z in range(ring)
    ]
    far = lax.ppermute(own, ("h", "z"), mirror)
    core = lax.ppermute(own, "k", swap)
    far_core = lax.ppermute(far, "k", swap)
    return own, core, far, far_core


def turned(array, shift):
    ring = lax.axis_size("z")
    return lax.ppermute(array, "z", [(i, (i + shift) % ring) for i in range(ring)])


def local(x, gain, embedding, request_span, passage_span, matching_pair, steepness):
    x = x[0]
    pairs = x.shape[0]
    ring = lax.axis_size("z")
    gain = gain[None]
    spans = (request_span, passage_span, matching_pair)
    plane = lax.axis_size(PLANE)
    normed = normalize(x, gain)
    slices = all_slices(embedding)
    q, copies, projected, emb = project(normed, slices, plane)
    queries = [q] + [turned(q, s) for s in range(1, ring)]
    docs = lax.all_to_all(copies, PLANE, split_axis=0, concat_axis=0, tiled=True)
    docs = docs.reshape(-1, docs.shape[-1])
    q_all, level, logits, stats = scores_forward(spans, steepness, docs, queries, pairs)
    stats = [stats] + [turned(stats, s) for s in range(1, ring)]
    gd, *parts, loss = slopes(
        spans, steepness, docs, q_all, level, logits, stats, pairs, copies.shape
    )
    grad_docs = lax.all_to_all(gd, PLANE, split_axis=0, concat_axis=0, tiled=True)
    grad_queries = [parts[0]] + [turned(parts[s], s) for s in range(1, ring)]
    grad_x = head_backward(x, gain, emb, projected, grad_docs, grad_queries)
    own = lax.dynamic_slice_in_dim(
        loss.reshape(ring, pairs, QLEN)[:, :, 0], lax.axis_index("z"), 1, 0
    )
    return grad_x[None], own


def solution(mesh):
    side = round(mesh.shape["dp"] ** (1 / 3))
    finer = Mesh(mesh.devices.reshape(2, 2, side, side, side), ("h", "k", "x", "y", "z"))
    rows = P(SECTION, DP, None, None)
    return jax.shard_map(
        local,
        mesh=finer,
        in_specs=(rows, P(), P(SECTION, None), P(), P(), P(), P()),
        out_specs=(rows, P(SECTION, DP)),
        check_vma=False,
    )
```

```python
import functools

import jax
import jax.numpy as jnp
from jax import lax
from jax.experimental import pallas as pl
from jax.experimental.pallas import tpu as pltpu
from jax.sharding import Mesh
from jax.sharding import PartitionSpec as P

QLEN = 32
DLEN = 64
LANES = 128
GROUP = 8
CHUNK = 512
DLEN_LEAST = 32
SECTION = ("h", "k")
PLANE = ("x", "y")
DP = ("x", "y", "z")

EPSILON = 1e-06
OBJECTIVE_FACTOR = 1024.0
MASKED = -1e30

LOG2_E = 1.4426950408889634
LN_2 = 0.6931471805599453

f32 = jnp.float32
bf16 = jnp.bfloat16


def grant(mib):
    return pltpu.CompilerParams(vmem_limit_bytes=mib * 1024 * 1024)


def vmem():
    return pl.BlockSpec(memory_space=pltpu.VMEM)


def hbm():
    return pl.BlockSpec(memory_space=pltpu.HBM)


def smem():
    return pl.BlockSpec(memory_space=pltpu.SMEM)


def dot_nt(a, b):
    return lax.dot_general(a, b, (((1,), (1,)), ((), ())), preferred_element_type=f32)


def dot_tn(a, b):
    return lax.dot_general(a, b, (((0,), (0,)), ((), ())), preferred_element_type=f32)


def in_turn(blocks, fill, use):
    fill(0, 0)
    for block in range(blocks):
        if block + 1 < blocks:
            fill(block + 1, (block + 1) % 2)
        use(block, block % 2)


def section_index():
    return lax.axis_index("h"), lax.axis_index("k")


def normalize_kernel(x_ref, gain_ref, normed_ref):
    values = x_ref[0].astype(f32)
    inverse_rms = lax.rsqrt(jnp.mean(values * values, axis=-1, keepdims=True) + EPSILON)
    normed_ref[0] = (values * inverse_rms * gain_ref[...]).astype(bf16)


def normalize(x, gain):
    pairs, length, width = x.shape
    rows = pl.BlockSpec((1, length, width), lambda i: (i, 0, 0))
    return pl.pallas_call(
        normalize_kernel,
        grid=(pairs,),
        in_specs=[rows, pl.BlockSpec((1, width), lambda i: (0, 0))],
        out_specs=rows,
        out_shape=jax.ShapeDtypeStruct(x.shape, bf16),
        compiler_params=grant(6),
        name="normalize",
    )(x, gain)


def project_kernel(normed_ref, own_ref, core_ref, far_ref, far_core_ref,
                   copies_ref, d_ref, proj_ref, emb_ref, q_ref, sems):
    depth = own_ref.shape[0]
    h, k = section_index()
    for ref, section in (
        (own_ref, h * 2 + k),
        (core_ref, h * 2 + 1 - k),
        (far_ref, (1 - h) * 2 + k),
        (far_core_ref, (1 - h) * 2 + 1 - k),
    ):
        emb_ref[pl.ds(pl.multiple_of(section * depth, depth), depth), :] = ref[...]
    pairs, _, _ = normed_ref.shape
    for p in range(pairs):
        projected = jnp.dot(normed_ref[p], emb_ref[...], preferred_element_type=f32)
        inverse_length = lax.rsqrt(
            jnp.sum(projected * projected, axis=-1, keepdims=True) + EPSILON
        )
        vectors = (projected * inverse_length).astype(bf16)
        q_ref[p * QLEN:(p + 1) * QLEN] = vectors[:QLEN]
        d_ref[p * DLEN:(p + 1) * DLEN] = vectors[QLEN:]
        proj_ref[p] = projected
    copies = [
        pltpu.make_async_copy(q_ref, copies_ref.at[n], sems.at[n])
        for n in range(copies_ref.shape[0])
    ]
    for copy in copies:
        copy.start()
    for copy in copies:
        copy.wait()


def project(normed, slices, readers):
    pairs, length, width = normed.shape
    _, features = slices[0].shape
    return pl.pallas_call(
        project_kernel,
        in_specs=[vmem()] * 5,
        out_specs=[hbm(), vmem(), vmem(), vmem()],
        out_shape=[
            pltpu.HBM((readers, pairs * QLEN, features), bf16),
            jax.ShapeDtypeStruct((pairs * DLEN, features), bf16),
            jax.ShapeDtypeStruct((pairs, length, features), f32),
            jax.ShapeDtypeStruct((width, features), bf16),
        ],
        scratch_shapes=[
            pltpu.VMEM((pairs * QLEN, features), bf16),
            pltpu.SemaphoreType.DMA((readers,)),
        ],
        compiler_params=grant(6),
        name="project",
    )(normed, *slices)


def micro_index():
    h, k = section_index()
    return h * 2 + k


def plane_index():
    return lax.axis_index("x") * lax.axis_size("y") + lax.axis_index("y")


def query_pair(holder, t, pairs):
    return (holder * lax.axis_size("z") + lax.axis_index("z")) * pairs + t


def document_pair(c, pairs, ring):
    z = lax.rem(lax.axis_index("z") - lax.div(c, pairs) + ring, ring)
    return (plane_index() * lax.axis_size("z") + z) * pairs + lax.rem(c, pairs)


def query_weights(request_ref, micro, holders, pairs):
    wide = pairs * QLEN
    lane = lax.broadcasted_iota(jnp.int32, (1, wide), 1)
    owner = lax.div(lane, QLEN)
    place = lane - owner * QLEN
    parts = []
    for holder in range(holders):
        span = jnp.zeros((1, wide), jnp.int32)
        for t in range(pairs):
            span = jnp.where(owner == t, request_ref[micro, query_pair(holder, t, pairs)], span)
        live = jnp.where(place < span, 1.0, 0.0).astype(f32)
        parts.append(live / span.astype(f32))
    return jnp.concatenate(parts, axis=1)


def matches(match_ref, micro, holders, pairs):
    lane = lax.broadcasted_iota(jnp.int32, (1, LANES), 1)
    match = jnp.full((1, LANES), -1, jnp.int32)
    for holder in range(holders):
        for t in range(pairs):
            match = jnp.where(
                lane == holder * pairs + t, match_ref[micro, query_pair(holder, t, pairs)], match
            )
    return match


def token_owners(lanes):
    first = lax.broadcasted_iota(jnp.int32, (lanes, LANES), 1) * QLEN
    ahead = lax.broadcasted_iota(jnp.int32, (lanes, LANES), 0) - first
    return jnp.where((ahead >= 0) & (ahead < QLEN), 1.0, 0.0).astype(bf16)


def parts_of(values):
    high = values.astype(bf16)
    rest = values - high.astype(f32)
    middle = rest.astype(bf16)
    low = (rest - middle.astype(f32)).astype(bf16)
    return low, middle, high


def sums_by_query(terms, owners):
    parts = [jnp.dot(part, owners, preferred_element_type=f32) for part in parts_of(terms)]
    return parts[0] + parts[1] + parts[2]


def given_to_tokens(values, owners):
    parts = [dot_nt(part, owners) for part in parts_of(values)]
    return parts[0] + parts[1] + parts[2]


def scores_kernel(pairs, request_ref, passage_ref, match_ref, steep_ref,
                  q_all, d0, d1, d2, d3,
                  docs_ref, level_ref, logits_ref, stats_ref, sim_a, sim_b):
    micro = micro_index()
    beta2 = steep_ref[0] * LOG2_E
    mult = steep_ref[1]
    arrived = (d0, d1, d2, d3)
    ring = len(arrived)
    own = d0.shape[0]
    for n, ref in enumerate(arrived):
        docs_ref[n * own:(n + 1) * own, :] = ref[...]
    lanes = q_all.shape[0]
    count = docs_ref.shape[0] // DLEN
    rows = GROUP * DLEN
    sims = (sim_a, sim_b)
    halves = count // GROUP
    token = lax.broadcasted_iota(jnp.int32, (DLEN - DLEN_LEAST, 1), 0) + DLEN_LEAST

    def spot(block):
        half, chunk = block % halves, block // halves
        return half * GROUP, slice(chunk * CHUNK, (chunk + 1) * CHUNK)

    def similarity(block, slot):
        c, at = spot(block)
        sims[slot][...] = dot_nt(docs_ref[c * DLEN:c * DLEN + rows, :], q_all[at, :])

    def pool(block, slot):
        ref = sims[slot]
        c, at = spot(block)
        levels = []
        for n in range(GROUP):
            span = passage_ref[micro, document_pair(c + n, pairs, ring)]
            row = n * DLEN
            early = ref[row:row + DLEN_LEAST, :]
            late = jnp.where(token < span, ref[row + DLEN_LEAST:row + DLEN, :], MASKED)
            highest = jnp.max(jnp.maximum(early, late), axis=0, keepdims=True)
            total = jnp.sum(
                jnp.exp2(beta2 * (early - highest)) + jnp.exp2(beta2 * (late - highest)),
                axis=0,
                keepdims=True,
            )
            levels.append(beta2 * highest + jnp.log2(total))
        level_ref[c:c + GROUP, at] = jnp.concatenate(levels, axis=0)

    in_turn(halves * (lanes // CHUNK), similarity, pool)

    holders = lanes // (pairs * QLEN)
    weight = query_weights(request_ref, micro, holders, pairs)
    smooth = level_ref[...] * (LN_2 / steep_ref[0])
    logits = mult * sums_by_query(smooth * weight, token_owners(lanes))
    logits_ref[...] = logits
    column = document_pair(lax.broadcasted_iota(jnp.int32, (count, 1), 0), pairs, ring)
    match = matches(match_ref, micro, holders, pairs)
    highest = jnp.max(logits, axis=0, keepdims=True)
    local = highest + jnp.log(jnp.sum(jnp.exp(logits - highest), axis=0, keepdims=True))
    positive = jnp.sum(jnp.where(column == match, logits, 0.0), axis=0, keepdims=True)
    tile = jnp.concatenate([local, positive, jnp.zeros((6, LANES), f32)], axis=0)
    for holder in range(holders):
        stats_ref[holder] = tile


def scores_forward(spans, steep, queries, docs, pairs):
    lanes, features = queries.shape
    rows = docs[0].shape[0] * len(docs)
    count = rows // DLEN
    holders = lanes // (pairs * QLEN)
    return pl.pallas_call(
        functools.partial(scores_kernel, pairs),
        in_specs=[smem()] * 4 + [vmem()] * 5,
        out_specs=[vmem()] * 4,
        out_shape=[
            jax.ShapeDtypeStruct((rows, features), bf16),
            jax.ShapeDtypeStruct((count, lanes), f32),
            jax.ShapeDtypeStruct((count, LANES), f32),
            jax.ShapeDtypeStruct((holders, 8, LANES), f32),
        ],
        scratch_shapes=[
            pltpu.VMEM((GROUP * DLEN, CHUNK), f32),
            pltpu.VMEM((GROUP * DLEN, CHUNK), f32),
        ],
        compiler_params=grant(10),
        name="scores_forward",
    )(*spans, steep, queries, *docs)


def slopes_kernel(pairs, ring, request_ref, passage_ref, match_ref, steep_ref,
                  docs_ref, q_all, level_ref, logits_ref, stats_ref,
                  gq_ref, gd0, gd1, gd2, gd3, loss_ref,
                  sim_a, sim_b, coef_ref, gq_vmem, sems):
    micro = micro_index()
    beta2 = steep_ref[0] * LOG2_E
    mult = steep_ref[1]
    lanes = q_all.shape[0]
    count = docs_ref.shape[0] // DLEN
    rows = GROUP * DLEN
    sims = (sim_a, sim_b)
    halves = count // GROUP
    holders = lanes // (pairs * QLEN)

    stats = stats_ref[...]
    locals_ = stats[:, 0, :]
    highest = jnp.max(locals_, axis=0, keepdims=True)
    log_total = highest + jnp.log(jnp.sum(jnp.exp(locals_ - highest), axis=0, keepdims=True))
    loss_ref[...] = log_total - jnp.sum(stats[:, 1, :], axis=0, keepdims=True)

    column = document_pair(lax.broadcasted_iota(jnp.int32, (count, 1), 0), pairs, ring)
    match = matches(match_ref, micro, holders, pairs)
    share = jnp.exp(logits_ref[...] - log_total) - jnp.where(column == match, 1.0, 0.0)
    slope = given_to_tokens(OBJECTIVE_FACTOR * mult * share, token_owners(lanes))
    coef_ref[...] = query_weights(request_ref, micro, holders, pairs) * slope

    token = lax.broadcasted_iota(jnp.int32, (DLEN - DLEN_LEAST, 1), 0) + DLEN_LEAST
    turned_parts = []
    sends = []
    gds = (gd0, gd1, gd2, gd3)
    own = gd0.shape[0]

    def spot(block):
        half, chunk = block % halves, block // halves
        return half * GROUP, slice(chunk * CHUNK, (chunk + 1) * CHUNK)

    def similarity(block, slot):
        c, at = spot(block)
        sims[slot][...] = dot_nt(docs_ref[c * DLEN:c * DLEN + rows, :], q_all[at, :])

    def weigh(block, slot):
        ref = sims[slot]
        c, at = spot(block)
        parts = []
        for n in range(GROUP):
            live = passage_ref[micro, document_pair(c + n, pairs, ring)]
            level = level_ref[c + n:c + n + 1, at]
            coef = coef_ref[c + n:c + n + 1, at]
            row = n * DLEN
            share = jnp.exp2(beta2 * ref[row:row + DLEN_LEAST, :] - level)
            parts.append((coef * share).astype(bf16))
            share = jnp.exp2(beta2 * ref[row + DLEN_LEAST:row + DLEN, :] - level)
            parts.append(jnp.where(token < live, coef * share, 0.0).astype(bf16))
        grad = jnp.concatenate(parts, axis=0)
        here = slice(c * DLEN, c * DLEN + rows)
        product = jnp.dot(grad, q_all[at, :], preferred_element_type=f32)
        for n in range(rows // own):
            ref = gds[c * DLEN // own + n]
            part = product[n * own:(n + 1) * own]
            ref[...] = part if block < halves else ref[...] + part
        turned_parts.append(dot_tn(docs_ref[here, :], grad))
        if len(turned_parts) == halves:
            total = functools.reduce(jnp.add, turned_parts)
            turned_parts.clear()
            gq_vmem[at, :] = total.T.astype(gq_vmem.dtype)
            send = pltpu.make_async_copy(
                gq_vmem.at[at], gq_ref.at[at], sems.at[block // halves]
            )
            send.start()
            sends.append(send)

    in_turn(halves * (lanes // CHUNK), similarity, weigh)
    for send in sends:
        send.wait()


def slopes(spans, steep, docs, queries, level, logits, stats, pairs, ring):
    lanes, features = queries.shape
    rows = docs.shape[0]
    return pl.pallas_call(
        functools.partial(slopes_kernel, pairs, ring),
        in_specs=[smem()] * 4 + [vmem()] * 5,
        out_specs=[hbm()] + [vmem()] * (ring + 1),
        out_shape=[
            pltpu.HBM((lanes, features), bf16),
            *[jax.ShapeDtypeStruct((rows // ring, features), f32)] * ring,
            jax.ShapeDtypeStruct((1, LANES), f32),
        ],
        scratch_shapes=[
            pltpu.VMEM((GROUP * DLEN, CHUNK), f32),
            pltpu.VMEM((GROUP * DLEN, CHUNK), f32),
            pltpu.VMEM(level.shape, f32),
            pltpu.VMEM((lanes, features), bf16),
            pltpu.SemaphoreType.DMA((lanes // CHUNK,)),
        ],
        compiler_params=grant(14),
        name="slopes",
    )(*spans, steep, docs, queries, level, logits, stats)


def head_backward_kernel(x_ref, gain_ref, emb_ref, proj_ref, gq_ref, g0, g1, g2, g3, out_ref,
                         out_vmem, sems):
    pairs = x_ref.shape[0]
    sends = []
    for p in range(pairs):
        at = slice(p * DLEN, (p + 1) * DLEN)
        grad_docs = g0[at] + g1[at] + g2[at] + g3[at]
        grad_query = jnp.sum(gq_ref[:, p * QLEN:(p + 1) * QLEN].astype(f32), axis=0)
        grad_vectors = jnp.concatenate([grad_query, grad_docs], axis=0)
        projected = proj_ref[p]
        inverse_length = lax.rsqrt(
            jnp.sum(projected * projected, axis=-1, keepdims=True) + EPSILON
        )
        unit = projected * inverse_length
        along = jnp.sum(unit * grad_vectors, axis=-1, keepdims=True)
        grad_projected = (inverse_length * (grad_vectors - unit * along)).astype(bf16)
        values = x_ref[p].astype(f32)
        inverse_rms = lax.rsqrt(jnp.mean(values * values, axis=-1, keepdims=True) + EPSILON)
        weighted = dot_nt(grad_projected, emb_ref[...]) * gain_ref[...]
        mean_term = jnp.mean(values * weighted, axis=-1, keepdims=True)
        out_vmem[p] = (
            inverse_rms * weighted
            - values * (inverse_rms * inverse_rms * inverse_rms) * mean_term
        ).astype(bf16)
        sends.append(pltpu.make_async_copy(out_vmem.at[p], out_ref.at[p], sems.at[p]))
        sends[-1].start()
    for send in sends:
        send.wait()


def head_backward(x, gain, emb, projected, grad_queries, grad_docs):
    pairs = x.shape[0]
    return pl.pallas_call(
        head_backward_kernel,
        in_specs=[vmem()] * 9,
        out_specs=hbm(),
        out_shape=jax.ShapeDtypeStruct(x.shape, bf16),
        scratch_shapes=[pltpu.VMEM(x.shape, bf16), pltpu.SemaphoreType.DMA((pairs,))],
        compiler_params=grant(10),
        name="head_backward",
    )(x, gain, emb, projected, grad_queries, *grad_docs)


def all_slices(own):
    swap = [(0, 1), (1, 0)]
    ring = lax.axis_size("z")
    mirror = [
        (h * ring + z, (1 - h) * ring + ring - 1 - z) for h in range(2) for z in range(ring)
    ]
    far = lax.ppermute(own, ("h", "z"), mirror)
    core = lax.ppermute(own, "k", swap)
    far_core = lax.ppermute(far, "k", swap)
    return own, core, far, far_core


def turned(array, shift):
    ring = lax.axis_size("z")
    return lax.ppermute(array, "z", [(i, (i + shift) % ring) for i in range(ring)])


def local(x, gain, embedding, request_span, passage_span, matching_pair, steepness):
    x = x[0]
    pairs = x.shape[0]
    ring = lax.axis_size("z")
    gain = gain[None]
    spans = (request_span, passage_span, matching_pair)
    plane = lax.axis_size(PLANE)

    def swapped(blocks):
        return lax.all_to_all(blocks, PLANE, split_axis=0, concat_axis=0, tiled=True)

    normed = normalize(x, gain)
    slices = all_slices(embedding)
    copies, d, projected, emb = project(normed, slices, plane)
    docs = [d] + [turned(d, s) for s in range(1, ring)]
    queries = swapped(copies)
    queries = queries.reshape(-1, queries.shape[-1])
    docs, level, logits, stats = scores_forward(spans, steepness, queries, docs, pairs)
    stats = swapped(stats)
    gq, *gd, loss = slopes(
        spans, steepness, docs, queries, level, logits, stats, pairs, ring
    )
    grad_docs = [gd[0]] + [turned(gd[s], -s) for s in range(1, ring)]
    grad_queries = swapped(gq.reshape(copies.shape))
    grad_x = head_backward(x, gain, emb, projected, grad_queries, grad_docs)
    own = lax.dynamic_slice_in_dim(loss, plane_index() * pairs, pairs, 1)
    return grad_x[None], own


def solution(mesh):
    side = round(mesh.shape["dp"] ** (1 / 3))
    finer = Mesh(mesh.devices.reshape(2, 2, side, side, side), ("h", "k", "x", "y", "z"))
    rows = P(SECTION, DP, None, None)
    return jax.shard_map(
        local,
        mesh=finer,
        in_specs=(rows, P(), P(SECTION, None), P(), P(), P(), P()),
        out_specs=(rows, P(SECTION, DP)),
        check_vma=False,
    )
```

```python
import functools

import jax
import jax.numpy as jnp
from jax import lax
from jax.experimental import pallas as pl
from jax.experimental.pallas import tpu as pltpu
from jax.sharding import Mesh
from jax.sharding import PartitionSpec as P

QLEN = 32
DLEN = 64
LANES = 128
GROUP = 8
CHUNK = 512
CHUNK_F = 2048
TOGETHER = 4
DLEN_LEAST = 32
SECTION = ("h", "k")
PLANE = ("x", "y")
DP = ("x", "y", "z")

EPSILON = 1e-06
OBJECTIVE_FACTOR = 1024.0
MASKED = -1e30

LOG2_E = 1.4426950408889634
LN_2 = 0.6931471805599453

f32 = jnp.float32
bf16 = jnp.bfloat16


def grant(mib):
    return pltpu.CompilerParams(vmem_limit_bytes=mib * 1024 * 1024)


def vmem():
    return pl.BlockSpec(memory_space=pltpu.VMEM)


def hbm():
    return pl.BlockSpec(memory_space=pltpu.HBM)


def smem():
    return pl.BlockSpec(memory_space=pltpu.SMEM)


def dot_nt(a, b):
    return lax.dot_general(a, b, (((1,), (1,)), ((), ())), preferred_element_type=f32)


def dot_tn(a, b):
    return lax.dot_general(a, b, (((0,), (0,)), ((), ())), preferred_element_type=f32)


def in_turn(blocks, fill, use):
    fill(0, 0)
    for block in range(blocks):
        if block + 1 < blocks:
            fill(block + 1, (block + 1) % 2)
        use(block, block % 2)


def section_index():
    return lax.axis_index("h"), lax.axis_index("k")


def normalize_kernel(x_ref, gain_ref, normed_ref):
    values = x_ref[0].astype(f32)
    inverse_rms = lax.rsqrt(jnp.mean(values * values, axis=-1, keepdims=True) + EPSILON)
    normed_ref[0] = (values * inverse_rms * gain_ref[...]).astype(bf16)


def normalize(x, gain):
    pairs, length, width = x.shape
    rows = pl.BlockSpec((1, length, width), lambda i: (i, 0, 0))
    return pl.pallas_call(
        normalize_kernel,
        grid=(pairs,),
        in_specs=[rows, pl.BlockSpec((1, width), lambda i: (0, 0))],
        out_specs=rows,
        out_shape=jax.ShapeDtypeStruct(x.shape, bf16),
        compiler_params=grant(6),
        name="normalize",
    )(x, gain)


def project_kernel(normed_ref, own_ref, core_ref, far_ref, far_core_ref,
                   copies_ref, d_ref, proj_ref, emb_ref, q_ref, sems):
    depth = own_ref.shape[0]
    h, k = section_index()
    for ref, section in (
        (own_ref, h * 2 + k),
        (core_ref, h * 2 + 1 - k),
        (far_ref, (1 - h) * 2 + k),
        (far_core_ref, (1 - h) * 2 + 1 - k),
    ):
        emb_ref[pl.ds(pl.multiple_of(section * depth, depth), depth), :] = ref[...]
    pairs, _, _ = normed_ref.shape
    for p in range(pairs):
        projected = jnp.dot(normed_ref[p], emb_ref[...], preferred_element_type=f32)
        inverse_length = lax.rsqrt(
            jnp.sum(projected * projected, axis=-1, keepdims=True) + EPSILON
        )
        vectors = (projected * inverse_length).astype(bf16)
        q_ref[p * QLEN:(p + 1) * QLEN] = vectors[:QLEN]
        d_ref[p * DLEN:(p + 1) * DLEN] = vectors[QLEN:]
        proj_ref[p] = projected
    copies = [
        pltpu.make_async_copy(q_ref, copies_ref.at[n], sems.at[n])
        for n in range(copies_ref.shape[0])
    ]
    for copy in copies:
        copy.start()
    for copy in copies:
        copy.wait()


def project(normed, slices, readers):
    pairs, length, width = normed.shape
    _, features = slices[0].shape
    return pl.pallas_call(
        project_kernel,
        in_specs=[vmem()] * 5,
        out_specs=[hbm(), vmem(), vmem(), vmem()],
        out_shape=[
            pltpu.HBM((readers, pairs * QLEN, features), bf16),
            jax.ShapeDtypeStruct((pairs * DLEN, features), bf16),
            jax.ShapeDtypeStruct((pairs, length, features), f32),
            jax.ShapeDtypeStruct((width, features), bf16),
        ],
        scratch_shapes=[
            pltpu.VMEM((pairs * QLEN, features), bf16),
            pltpu.SemaphoreType.DMA((readers,)),
        ],
        compiler_params=grant(6),
        name="project",
    )(normed, *slices)


def micro_index():
    h, k = section_index()
    return h * 2 + k


def plane_index():
    return lax.axis_index("x") * lax.axis_size("y") + lax.axis_index("y")


def query_pair(holder, t, pairs):
    return (holder * lax.axis_size("z") + lax.axis_index("z")) * pairs + t


def document_pair(c, pairs):
    z = jnp.bitwise_xor(lax.axis_index("z"), lax.div(c, pairs))
    return (plane_index() * lax.axis_size("z") + z) * pairs + lax.rem(c, pairs)


def query_weights(request_ref, micro, holders, pairs):
    wide = pairs * QLEN
    lane = lax.broadcasted_iota(jnp.int32, (1, wide), 1)
    owner = lax.div(lane, QLEN)
    place = lane - owner * QLEN
    parts = []
    for holder in range(holders):
        span = jnp.zeros((1, wide), jnp.int32)
        for t in range(pairs):
            span = jnp.where(owner == t, request_ref[micro, query_pair(holder, t, pairs)], span)
        live = jnp.where(place < span, 1.0, 0.0).astype(f32)
        parts.append(live / span.astype(f32))
    return jnp.concatenate(parts, axis=1)


def matches(match_ref, micro, holders, pairs):
    lane = lax.broadcasted_iota(jnp.int32, (1, LANES), 1)
    match = jnp.full((1, LANES), -1, jnp.int32)
    for holder in range(holders):
        for t in range(pairs):
            match = jnp.where(
                lane == holder * pairs + t, match_ref[micro, query_pair(holder, t, pairs)], match
            )
    return match


def first_owners():
    start = lax.broadcasted_iota(jnp.int32, (LANES, LANES), 0) * QLEN
    ahead = lax.broadcasted_iota(jnp.int32, (LANES, LANES), 1) - start
    return jnp.where((ahead >= 0) & (ahead < QLEN), 1.0, 0.0).astype(bf16)


def parts_of(values):
    high = values.astype(bf16)
    rest = values - high.astype(f32)
    middle = rest.astype(bf16)
    low = (rest - middle.astype(f32)).astype(bf16)
    return jnp.concatenate([low, middle, high], axis=0)


def joined(parts):
    rows = parts.shape[0] // 3
    return parts[:rows] + parts[rows:2 * rows] + parts[2 * rows:]


def sums_by_query(terms, pairs):
    wide = pairs * QLEN
    owners = first_owners()
    total = None
    for holder in range(terms.shape[1] // wide):
        sums = joined(dot_nt(parts_of(terms[:, holder * wide:(holder + 1) * wide]), owners))
        sums = pltpu.roll(sums, holder * pairs, 1) if holder else sums
        total = sums if total is None else total + sums
    return total


def given_to_tokens(values, holders, pairs):
    owners = first_owners()
    given = []
    for holder in range(holders):
        own = pltpu.roll(values, LANES - holder * pairs, 1) if holder else values
        given.append(joined(jnp.dot(parts_of(own), owners, preferred_element_type=f32)))
    return jnp.concatenate(given, axis=1)


def scores_kernel(pairs, request_ref, passage_ref, match_ref, steep_ref,
                  q_all, d0, d1, d2, d3,
                  docs_ref, level_ref, logits_ref, stats_ref, sim_a, sim_b):
    micro = micro_index()
    beta2 = steep_ref[0] * LOG2_E
    mult = steep_ref[1]
    arrived = (d0, d1, d2, d3)
    own = d0.shape[0]
    for n, ref in enumerate(arrived):
        docs_ref[n * own:(n + 1) * own, :] = ref[...]
    lanes = q_all.shape[0]
    count = docs_ref.shape[0] // DLEN
    rows = GROUP * DLEN
    sims = (sim_a, sim_b)
    halves = count // GROUP
    token = lax.broadcasted_iota(jnp.int32, (DLEN - DLEN_LEAST, 1), 0) + DLEN_LEAST

    def spot(block):
        half, chunk = block % halves, block // halves
        return half * GROUP, slice(chunk * CHUNK_F, (chunk + 1) * CHUNK_F)

    def similarity(block, slot):
        c, at = spot(block)
        sims[slot][...] = dot_nt(docs_ref[c * DLEN:c * DLEN + rows, :], q_all[at, :])

    def pool(block, slot):
        ref = sims[slot]
        c, at = spot(block)
        levels = []
        for n in range(GROUP):
            span = passage_ref[micro, document_pair(c + n, pairs)]
            row = n * DLEN
            early = ref[row:row + DLEN_LEAST, :]
            late = jnp.where(token < span, ref[row + DLEN_LEAST:row + DLEN, :], MASKED)
            highest = jnp.max(jnp.maximum(early, late), axis=0, keepdims=True)
            total = jnp.sum(
                jnp.exp2(beta2 * (early - highest)) + jnp.exp2(beta2 * (late - highest)),
                axis=0,
                keepdims=True,
            )
            levels.append(beta2 * highest + jnp.log2(total))
        level_ref[c:c + GROUP, at] = jnp.concatenate(levels, axis=0)

    in_turn(halves * (lanes // CHUNK_F), similarity, pool)

    holders = lanes // (pairs * QLEN)
    weight = query_weights(request_ref, micro, holders, pairs)
    smooth = level_ref[...] * (LN_2 / steep_ref[0])
    logits = mult * sums_by_query(smooth * weight, pairs)
    logits_ref[...] = logits
    column = document_pair(lax.broadcasted_iota(jnp.int32, (count, 1), 0), pairs)
    match = matches(match_ref, micro, holders, pairs)
    highest = jnp.max(logits, axis=0, keepdims=True)
    local = highest + jnp.log(jnp.sum(jnp.exp(logits - highest), axis=0, keepdims=True))
    positive = jnp.sum(jnp.where(column == match, logits, 0.0), axis=0, keepdims=True)
    tile = jnp.concatenate([local, positive, jnp.zeros((6, LANES), f32)], axis=0)
    for holder in range(holders):
        stats_ref[holder] = tile


def scores_forward(spans, steep, queries, docs, pairs):
    lanes, features = queries.shape
    rows = docs[0].shape[0] * len(docs)
    count = rows // DLEN
    holders = lanes // (pairs * QLEN)
    return pl.pallas_call(
        functools.partial(scores_kernel, pairs),
        in_specs=[smem()] * 4 + [vmem()] * 5,
        out_specs=[vmem()] * 4,
        out_shape=[
            jax.ShapeDtypeStruct((rows, features), bf16),
            jax.ShapeDtypeStruct((count, lanes), f32),
            jax.ShapeDtypeStruct((count, LANES), f32),
            jax.ShapeDtypeStruct((holders, 8, LANES), f32),
        ],
        scratch_shapes=[
            pltpu.VMEM((GROUP * DLEN, CHUNK_F), f32),
            pltpu.VMEM((GROUP * DLEN, CHUNK_F), f32),
        ],
        compiler_params=grant(10),
        name="scores_forward",
    )(*spans, steep, queries, *docs)


def slopes_kernel(pairs, request_ref, passage_ref, match_ref, steep_ref,
                  docs_ref, q_all, level_ref, logits_ref, stats_ref,
                  gq_ref, gd0, gd1, gd2, gd3, loss_ref,
                  sim_a, sim_b, coef_ref, gq_vmem, sems):
    micro = micro_index()
    beta2 = steep_ref[0] * LOG2_E
    mult = steep_ref[1]
    lanes = q_all.shape[0]
    count = docs_ref.shape[0] // DLEN
    rows = GROUP * DLEN
    sims = (sim_a, sim_b)
    halves = count // GROUP
    holders = lanes // (pairs * QLEN)

    stats = stats_ref[...]
    locals_ = stats[:, 0, :]
    highest = jnp.max(locals_, axis=0, keepdims=True)
    log_total = highest + jnp.log(jnp.sum(jnp.exp(locals_ - highest), axis=0, keepdims=True))
    loss_ref[...] = log_total - jnp.sum(stats[:, 1, :], axis=0, keepdims=True)

    column = document_pair(lax.broadcasted_iota(jnp.int32, (count, 1), 0), pairs)
    match = matches(match_ref, micro, holders, pairs)
    share = jnp.exp(logits_ref[...] - log_total) - jnp.where(column == match, 1.0, 0.0)
    slope = given_to_tokens(OBJECTIVE_FACTOR * mult * share, holders, pairs)
    coef_ref[...] = query_weights(request_ref, micro, holders, pairs) * slope

    token = lax.broadcasted_iota(jnp.int32, (DLEN - DLEN_LEAST, 1), 0) + DLEN_LEAST
    turned_parts = []
    sends = []
    gds = (gd0, gd1, gd2, gd3)
    own = gd0.shape[0]

    def spot(block):
        half, chunk = block % halves, block // halves
        return half * GROUP, slice(chunk * CHUNK, (chunk + 1) * CHUNK)

    def similarity(block, slot):
        c, at = spot(block)
        sims[slot][...] = dot_nt(docs_ref[c * DLEN:c * DLEN + rows, :], q_all[at, :])

    def weigh(block, slot):
        ref = sims[slot]
        c, at = spot(block)
        parts = []
        for n in range(GROUP):
            live = passage_ref[micro, document_pair(c + n, pairs)]
            level = level_ref[c + n:c + n + 1, at]
            coef = coef_ref[c + n:c + n + 1, at]
            row = n * DLEN
            share = jnp.exp2(beta2 * ref[row:row + DLEN_LEAST, :] - level)
            parts.append((coef * share).astype(bf16))
            share = jnp.exp2(beta2 * ref[row + DLEN_LEAST:row + DLEN, :] - level)
            parts.append(jnp.where(token < live, coef * share, 0.0).astype(bf16))
        grad = jnp.concatenate(parts, axis=0)
        here = slice(c * DLEN, c * DLEN + rows)
        product = jnp.dot(grad, q_all[at, :], preferred_element_type=f32)
        for n in range(rows // own):
            ref = gds[c * DLEN // own + n]
            part = product[n * own:(n + 1) * own]
            ref[...] = part if block < halves else ref[...] + part
        turned_parts.append(dot_tn(docs_ref[here, :], grad))
        if len(turned_parts) == halves:
            total = functools.reduce(jnp.add, turned_parts)
            turned_parts.clear()
            gq_vmem[at, :] = total.T.astype(gq_vmem.dtype)
            send = pltpu.make_async_copy(
                gq_vmem.at[at], gq_ref.at[at], sems.at[block // halves]
            )
            send.start()
            sends.append(send)

    in_turn(halves * (lanes // CHUNK), similarity, weigh)
    for send in sends:
        send.wait()


def slopes(spans, steep, docs, queries, level, logits, stats, pairs, ring):
    lanes, features = queries.shape
    rows = docs.shape[0]
    return pl.pallas_call(
        functools.partial(slopes_kernel, pairs),
        in_specs=[smem()] * 4 + [vmem()] * 5,
        out_specs=[hbm()] + [vmem()] * (ring + 1),
        out_shape=[
            pltpu.HBM((lanes, features), bf16),
            *[jax.ShapeDtypeStruct((rows // ring, features), f32)] * ring,
            jax.ShapeDtypeStruct((1, LANES), f32),
        ],
        scratch_shapes=[
            pltpu.VMEM((GROUP * DLEN, CHUNK), f32),
            pltpu.VMEM((GROUP * DLEN, CHUNK), f32),
            pltpu.VMEM(level.shape, f32),
            pltpu.VMEM((lanes, features), bf16),
            pltpu.SemaphoreType.DMA((lanes // CHUNK,)),
        ],
        compiler_params=grant(14),
        name="slopes",
    )(*spans, steep, docs, queries, level, logits, stats)


def head_backward_kernel(x_ref, gain_ref, emb_ref, proj_ref, gq_ref, g0, g1, g2, g3, out_ref,
                         out_vmem, sems):
    pairs = x_ref.shape[0]
    sends = []
    for first in range(0, pairs, TOGETHER):
        group = range(first, first + TOGETHER)
        grads = []
        for p in group:
            at = slice(p * DLEN, (p + 1) * DLEN)
            grad_docs = g0[at] + g1[at] + g2[at] + g3[at]
            grad_query = jnp.sum(gq_ref[:, p * QLEN:(p + 1) * QLEN].astype(f32), axis=0)
            grad_vectors = jnp.concatenate([grad_query, grad_docs], axis=0)
            projected = proj_ref[p]
            inverse_length = lax.rsqrt(
                jnp.sum(projected * projected, axis=-1, keepdims=True) + EPSILON
            )
            unit = projected * inverse_length
            along = jnp.sum(unit * grad_vectors, axis=-1, keepdims=True)
            grads.append((inverse_length * (grad_vectors - unit * along)).astype(bf16))
        normed = dot_nt(jnp.concatenate(grads, axis=0), emb_ref[...])
        rows = normed.shape[0] // TOGETHER
        for n, p in enumerate(group):
            values = x_ref[p].astype(f32)
            inverse_rms = lax.rsqrt(jnp.mean(values * values, axis=-1, keepdims=True) + EPSILON)
            weighted = normed[n * rows:(n + 1) * rows] * gain_ref[...]
            mean_term = jnp.mean(values * weighted, axis=-1, keepdims=True)
            out_vmem[p] = (
                inverse_rms * weighted
                - values * (inverse_rms * inverse_rms * inverse_rms) * mean_term
            ).astype(bf16)
            sends.append(pltpu.make_async_copy(out_vmem.at[p], out_ref.at[p], sems.at[p]))
            sends[-1].start()
    for send in sends:
        send.wait()


def head_backward(x, gain, emb, projected, grad_queries, grad_docs):
    pairs = x.shape[0]
    return pl.pallas_call(
        head_backward_kernel,
        in_specs=[vmem()] * 9,
        out_specs=hbm(),
        out_shape=jax.ShapeDtypeStruct(x.shape, bf16),
        scratch_shapes=[pltpu.VMEM(x.shape, bf16), pltpu.SemaphoreType.DMA((pairs,))],
        compiler_params=grant(14),
        name="head_backward",
    )(x, gain, emb, projected, grad_queries, *grad_docs)


def all_slices(own):
    swap = [(0, 1), (1, 0)]
    ring = lax.axis_size("z")
    mirror = [
        (h * ring + z, (1 - h) * ring + ring - 1 - z) for h in range(2) for z in range(ring)
    ]
    far = lax.ppermute(own, ("h", "z"), mirror)
    core = lax.ppermute(own, "k", swap)
    far_core = lax.ppermute(far, "k", swap)
    return own, core, far, far_core


def traded(array, step):
    return lax.ppermute(array, "z", [(i, i ^ step) for i in range(lax.axis_size("z"))])


def local(x, gain, embedding, request_span, passage_span, matching_pair, steepness):
    x = x[0]
    pairs = x.shape[0]
    ring = lax.axis_size("z")
    gain = gain[None]
    spans = (request_span, passage_span, matching_pair)
    plane = lax.axis_size(PLANE)

    def swapped(blocks):
        return lax.all_to_all(blocks, PLANE, split_axis=0, concat_axis=0, tiled=True)

    normed = normalize(x, gain)
    slices = all_slices(embedding)
    copies, d, projected, emb = project(normed, slices, plane)
    docs = [d] + [traded(d, s) for s in range(1, ring)]
    queries = swapped(copies)
    queries = queries.reshape(-1, queries.shape[-1])
    docs, level, logits, stats = scores_forward(spans, steepness, queries, docs, pairs)
    stats = swapped(stats)
    gq, *gd, loss = slopes(
        spans, steepness, docs, queries, level, logits, stats, pairs, ring
    )
    grad_docs = [gd[0]] + [traded(gd[s], s) for s in range(1, ring)]
    grad_queries = swapped(gq.reshape(copies.shape))
    grad_x = head_backward(x, gain, emb, projected, grad_queries, grad_docs)
    own = lax.dynamic_slice_in_dim(loss, plane_index() * pairs, pairs, 1)
    return grad_x[None], own


def solution(mesh):
    side = round(mesh.shape["dp"] ** (1 / 3))
    finer = Mesh(mesh.devices.reshape(2, 2, side, side, side), ("h", "k", "x", "y", "z"))
    rows = P(SECTION, DP, None, None)
    return jax.shard_map(
        local,
        mesh=finer,
        in_specs=(rows, P(), P(SECTION, None), P(), P(), P(), P()),
        out_specs=(rows, P(SECTION, DP)),
        check_vma=False,
    )
```

```python
import functools

import jax
import jax.numpy as jnp
from jax import lax
from jax.experimental import pallas as pl
from jax.experimental.pallas import tpu as pltpu
from jax.sharding import Mesh
from jax.sharding import PartitionSpec as P

QLEN = 32
DLEN = 64
LANES = 128
GROUP = 8
CHUNK = 512
CHUNK_F = 2048
TOGETHER = 4
DLEN_LEAST = 32
SECTION = ("h", "k")
PLANE = ("x", "y")
DP = ("x", "y", "z")

EPSILON = 1e-06
OBJECTIVE_FACTOR = 1024.0
MASKED = -1e30

LOG2_E = 1.4426950408889634
LN_2 = 0.6931471805599453

f32 = jnp.float32
bf16 = jnp.bfloat16


def grant(mib):
    return pltpu.CompilerParams(vmem_limit_bytes=mib * 1024 * 1024)


def vmem():
    return pl.BlockSpec(memory_space=pltpu.VMEM)


def hbm():
    return pl.BlockSpec(memory_space=pltpu.HBM)


def smem():
    return pl.BlockSpec(memory_space=pltpu.SMEM)


def dot_nt(a, b):
    return lax.dot_general(a, b, (((1,), (1,)), ((), ())), preferred_element_type=f32)


def dot_tn(a, b):
    return lax.dot_general(a, b, (((0,), (0,)), ((), ())), preferred_element_type=f32)


def in_turn(blocks, fill, use):
    fill(0, 0)
    for block in range(blocks):
        if block + 1 < blocks:
            fill(block + 1, (block + 1) % 2)
        use(block, block % 2)


def section_index():
    return lax.axis_index("h"), lax.axis_index("k")


def normalize_kernel(x_ref, gain_ref, normed_ref):
    values = x_ref[0].astype(f32)
    inverse_rms = lax.rsqrt(jnp.mean(values * values, axis=-1, keepdims=True) + EPSILON)
    normed_ref[0] = (values * inverse_rms * gain_ref[...]).astype(bf16)


def normalize(x, gain):
    pairs, length, width = x.shape
    rows = pl.BlockSpec((1, length, width), lambda i: (i, 0, 0))
    return pl.pallas_call(
        normalize_kernel,
        grid=(pairs,),
        in_specs=[rows, pl.BlockSpec((1, width), lambda i: (0, 0))],
        out_specs=rows,
        out_shape=jax.ShapeDtypeStruct(x.shape, bf16),
        compiler_params=grant(6),
        name="normalize",
    )(x, gain)


def section_rows(depth, far, other):
    h, k = section_index()
    section = (1 - h if far else h) * 2 + (1 - k if other else k)
    return pl.ds(pl.multiple_of(section * depth, depth), depth)


def partial_kernel(normed_ref, own_ref, core_ref, far_ref, part_ref):
    depth = own_ref.shape[0]
    for p in range(normed_ref.shape[0]):
        part_ref[p] = sum(
            jnp.dot(normed_ref[p, :, section_rows(depth, far, other)], ref[...],
                    preferred_element_type=f32)
            for ref, far, other in ((own_ref, 0, 0), (core_ref, 0, 1), (far_ref, 1, 0))
        )


def project_partly(normed, own, core, far):
    pairs, length, _ = normed.shape
    return pl.pallas_call(
        partial_kernel,
        in_specs=[vmem()] * 4,
        out_specs=vmem(),
        out_shape=jax.ShapeDtypeStruct((pairs, length, own.shape[1]), f32),
        compiler_params=grant(6),
        name="project_partly",
    )(normed, own, core, far)


def project_kernel(normed_ref, part_ref, last_ref, copies_ref, d_ref, proj_ref, q_ref, sems):
    depth = last_ref.shape[0]
    for p in range(normed_ref.shape[0]):
        projected = part_ref[p] + jnp.dot(
            normed_ref[p, :, section_rows(depth, 1, 1)], last_ref[...],
            preferred_element_type=f32,
        )
        inverse_length = lax.rsqrt(
            jnp.sum(projected * projected, axis=-1, keepdims=True) + EPSILON
        )
        vectors = (projected * inverse_length).astype(bf16)
        q_ref[p * QLEN:(p + 1) * QLEN] = vectors[:QLEN]
        d_ref[p * DLEN:(p + 1) * DLEN] = vectors[QLEN:]
        proj_ref[p] = projected
    copies = [
        pltpu.make_async_copy(q_ref, copies_ref.at[n], sems.at[n])
        for n in range(copies_ref.shape[0])
    ]
    for copy in copies:
        copy.start()
    for copy in copies:
        copy.wait()


def project(normed, part, last, readers):
    pairs, length, _ = normed.shape
    features = last.shape[1]
    return pl.pallas_call(
        project_kernel,
        in_specs=[vmem()] * 3,
        out_specs=[hbm(), vmem(), vmem()],
        out_shape=[
            pltpu.HBM((readers, pairs * QLEN, features), bf16),
            jax.ShapeDtypeStruct((pairs * DLEN, features), bf16),
            jax.ShapeDtypeStruct((pairs, length, features), f32),
        ],
        scratch_shapes=[
            pltpu.VMEM((pairs * QLEN, features), bf16),
            pltpu.SemaphoreType.DMA((readers,)),
        ],
        compiler_params=grant(6),
        name="project",
    )(normed, part, last)


def assemble_kernel(own_ref, core_ref, far_ref, far_core_ref, emb_ref):
    depth = own_ref.shape[0]
    emb_ref[section_rows(depth, 0, 0), :] = own_ref[...]
    emb_ref[section_rows(depth, 0, 1), :] = core_ref[...]
    emb_ref[section_rows(depth, 1, 0), :] = far_ref[...]
    emb_ref[section_rows(depth, 1, 1), :] = far_core_ref[...]


def assemble(slices):
    depth, features = slices[0].shape
    return pl.pallas_call(
        assemble_kernel,
        in_specs=[vmem()] * 4,
        out_specs=vmem(),
        out_shape=jax.ShapeDtypeStruct((depth * len(slices), features), bf16),
        compiler_params=grant(4),
        name="assemble",
    )(*slices)


def micro_index():
    h, k = section_index()
    return h * 2 + k


def plane_index():
    return lax.axis_index("x") * lax.axis_size("y") + lax.axis_index("y")


def query_pair(holder, t, pairs):
    return (holder * lax.axis_size("z") + lax.axis_index("z")) * pairs + t


def document_pair(c, pairs):
    z = jnp.bitwise_xor(lax.axis_index("z"), lax.div(c, pairs))
    return (plane_index() * lax.axis_size("z") + z) * pairs + lax.rem(c, pairs)


def query_weights(request_ref, micro, holders, pairs):
    wide = pairs * QLEN
    lane = lax.broadcasted_iota(jnp.int32, (1, wide), 1)
    owner = lax.div(lane, QLEN)
    place = lane - owner * QLEN
    parts = []
    for holder in range(holders):
        span = jnp.zeros((1, wide), jnp.int32)
        for t in range(pairs):
            span = jnp.where(owner == t, request_ref[micro, query_pair(holder, t, pairs)], span)
        live = jnp.where(place < span, 1.0, 0.0).astype(f32)
        parts.append(live / span.astype(f32))
    return jnp.concatenate(parts, axis=1)


def matches(match_ref, micro, holders, pairs):
    lane = lax.broadcasted_iota(jnp.int32, (1, LANES), 1)
    match = jnp.full((1, LANES), -1, jnp.int32)
    for holder in range(holders):
        for t in range(pairs):
            match = jnp.where(
                lane == holder * pairs + t, match_ref[micro, query_pair(holder, t, pairs)], match
            )
    return match


def first_owners():
    start = lax.broadcasted_iota(jnp.int32, (LANES, LANES), 0) * QLEN
    ahead = lax.broadcasted_iota(jnp.int32, (LANES, LANES), 1) - start
    return jnp.where((ahead >= 0) & (ahead < QLEN), 1.0, 0.0).astype(bf16)


def parts_of(values):
    high = values.astype(bf16)
    rest = values - high.astype(f32)
    middle = rest.astype(bf16)
    low = (rest - middle.astype(f32)).astype(bf16)
    return jnp.concatenate([low, middle, high], axis=0)


def joined(parts):
    rows = parts.shape[0] // 3
    return parts[:rows] + parts[rows:2 * rows] + parts[2 * rows:]


def sums_by_query(terms, pairs):
    wide = pairs * QLEN
    owners = first_owners()
    total = None
    for holder in range(terms.shape[1] // wide):
        sums = joined(dot_nt(parts_of(terms[:, holder * wide:(holder + 1) * wide]), owners))
        sums = pltpu.roll(sums, holder * pairs, 1) if holder else sums
        total = sums if total is None else total + sums
    return total


def given_to_tokens(values, holders, pairs):
    owners = first_owners()
    given = []
    for holder in range(holders):
        own = pltpu.roll(values, LANES - holder * pairs, 1) if holder else values
        given.append(joined(jnp.dot(parts_of(own), owners, preferred_element_type=f32)))
    return jnp.concatenate(given, axis=1)


def scores_kernel(pairs, request_ref, passage_ref, match_ref, steep_ref,
                  q_all, d0, d1, d2, d3,
                  docs_ref, level_ref, logits_ref, stats_ref, sim_a, sim_b):
    micro = micro_index()
    beta2 = steep_ref[0] * LOG2_E
    mult = steep_ref[1]
    arrived = (d0, d1, d2, d3)
    own = d0.shape[0]
    for n, ref in enumerate(arrived):
        docs_ref[n * own:(n + 1) * own, :] = ref[...]
    lanes = q_all.shape[0]
    count = docs_ref.shape[0] // DLEN
    rows = GROUP * DLEN
    sims = (sim_a, sim_b)
    halves = count // GROUP
    token = lax.broadcasted_iota(jnp.int32, (DLEN - DLEN_LEAST, 1), 0) + DLEN_LEAST

    def spot(block):
        half, chunk = block % halves, block // halves
        return half * GROUP, slice(chunk * CHUNK_F, (chunk + 1) * CHUNK_F)

    def similarity(block, slot):
        c, at = spot(block)
        sims[slot][...] = dot_nt(docs_ref[c * DLEN:c * DLEN + rows, :], q_all[at, :])

    def pool(block, slot):
        ref = sims[slot]
        c, at = spot(block)
        levels = []
        for n in range(GROUP):
            span = passage_ref[micro, document_pair(c + n, pairs)]
            row = n * DLEN
            early = ref[row:row + DLEN_LEAST, :]
            late = jnp.where(token < span, ref[row + DLEN_LEAST:row + DLEN, :], MASKED)
            highest = jnp.max(jnp.maximum(early, late), axis=0, keepdims=True)
            total = jnp.sum(
                jnp.exp2(beta2 * (early - highest)) + jnp.exp2(beta2 * (late - highest)),
                axis=0,
                keepdims=True,
            )
            levels.append(beta2 * highest + jnp.log2(total))
        level_ref[c:c + GROUP, at] = jnp.concatenate(levels, axis=0)

    in_turn(halves * (lanes // CHUNK_F), similarity, pool)

    holders = lanes // (pairs * QLEN)
    weight = query_weights(request_ref, micro, holders, pairs)
    smooth = level_ref[...] * (LN_2 / steep_ref[0])
    logits = mult * sums_by_query(smooth * weight, pairs)
    logits_ref[...] = logits
    column = document_pair(lax.broadcasted_iota(jnp.int32, (count, 1), 0), pairs)
    match = matches(match_ref, micro, holders, pairs)
    highest = jnp.max(logits, axis=0, keepdims=True)
    local = highest + jnp.log(jnp.sum(jnp.exp(logits - highest), axis=0, keepdims=True))
    positive = jnp.sum(jnp.where(column == match, logits, 0.0), axis=0, keepdims=True)
    tile = jnp.concatenate([local, positive, jnp.zeros((6, LANES), f32)], axis=0)
    for holder in range(holders):
        stats_ref[holder] = tile


def scores_forward(spans, steep, queries, docs, pairs):
    lanes, features = queries.shape
    rows = docs[0].shape[0] * len(docs)
    count = rows // DLEN
    holders = lanes // (pairs * QLEN)
    return pl.pallas_call(
        functools.partial(scores_kernel, pairs),
        in_specs=[smem()] * 4 + [vmem()] * 5,
        out_specs=[vmem()] * 4,
        out_shape=[
            jax.ShapeDtypeStruct((rows, features), bf16),
            jax.ShapeDtypeStruct((count, lanes), f32),
            jax.ShapeDtypeStruct((count, LANES), f32),
            jax.ShapeDtypeStruct((holders, 8, LANES), f32),
        ],
        scratch_shapes=[
            pltpu.VMEM((GROUP * DLEN, CHUNK_F), f32),
            pltpu.VMEM((GROUP * DLEN, CHUNK_F), f32),
        ],
        compiler_params=grant(10),
        name="scores_forward",
    )(*spans, steep, queries, *docs)


def slopes_kernel(pairs, request_ref, passage_ref, match_ref, steep_ref,
                  docs_ref, q_all, level_ref, logits_ref, stats_ref,
                  gq_ref, gd0, gd1, gd2, gd3, loss_ref,
                  sim_a, sim_b, coef_ref, gq_vmem, sems):
    micro = micro_index()
    beta2 = steep_ref[0] * LOG2_E
    mult = steep_ref[1]
    lanes = q_all.shape[0]
    count = docs_ref.shape[0] // DLEN
    rows = GROUP * DLEN
    sims = (sim_a, sim_b)
    halves = count // GROUP
    holders = lanes // (pairs * QLEN)

    stats = stats_ref[...]
    locals_ = stats[:, 0, :]
    highest = jnp.max(locals_, axis=0, keepdims=True)
    log_total = highest + jnp.log(jnp.sum(jnp.exp(locals_ - highest), axis=0, keepdims=True))
    loss_ref[...] = log_total - jnp.sum(stats[:, 1, :], axis=0, keepdims=True)

    column = document_pair(lax.broadcasted_iota(jnp.int32, (count, 1), 0), pairs)
    match = matches(match_ref, micro, holders, pairs)
    share = jnp.exp(logits_ref[...] - log_total) - jnp.where(column == match, 1.0, 0.0)
    slope = given_to_tokens(OBJECTIVE_FACTOR * mult * share, holders, pairs)
    coef_ref[...] = query_weights(request_ref, micro, holders, pairs) * slope

    token = lax.broadcasted_iota(jnp.int32, (DLEN - DLEN_LEAST, 1), 0) + DLEN_LEAST
    turned_parts = []
    sends = []
    gds = (gd0, gd1, gd2, gd3)
    own = gd0.shape[0]

    def spot(block):
        half, chunk = block % halves, block // halves
        return half * GROUP, slice(chunk * CHUNK, (chunk + 1) * CHUNK)

    def similarity(block, slot):
        c, at = spot(block)
        sims[slot][...] = dot_nt(docs_ref[c * DLEN:c * DLEN + rows, :], q_all[at, :])

    def weigh(block, slot):
        ref = sims[slot]
        c, at = spot(block)
        parts = []
        for n in range(GROUP):
            live = passage_ref[micro, document_pair(c + n, pairs)]
            level = level_ref[c + n:c + n + 1, at]
            coef = coef_ref[c + n:c + n + 1, at]
            row = n * DLEN
            share = jnp.exp2(beta2 * ref[row:row + DLEN_LEAST, :] - level)
            parts.append((coef * share).astype(bf16))
            share = jnp.exp2(beta2 * ref[row + DLEN_LEAST:row + DLEN, :] - level)
            parts.append(jnp.where(token < live, coef * share, 0.0).astype(bf16))
        grad = jnp.concatenate(parts, axis=0)
        here = slice(c * DLEN, c * DLEN + rows)
        product = jnp.dot(grad, q_all[at, :], preferred_element_type=f32)
        for n in range(rows // own):
            ref = gds[c * DLEN // own + n]
            part = product[n * own:(n + 1) * own]
            ref[...] = part if block < halves else ref[...] + part
        turned_parts.append(dot_tn(docs_ref[here, :], grad))
        if len(turned_parts) == halves:
            total = functools.reduce(jnp.add, turned_parts)
            turned_parts.clear()
            gq_vmem[at, :] = total.T.astype(gq_vmem.dtype)
            send = pltpu.make_async_copy(
                gq_vmem.at[at], gq_ref.at[at], sems.at[block // halves]
            )
            send.start()
            sends.append(send)

    in_turn(halves * (lanes // CHUNK), similarity, weigh)
    for send in sends:
        send.wait()


def slopes(spans, steep, docs, queries, level, logits, stats, pairs, ring):
    lanes, features = queries.shape
    rows = docs.shape[0]
    return pl.pallas_call(
        functools.partial(slopes_kernel, pairs),
        in_specs=[smem()] * 4 + [vmem()] * 5,
        out_specs=[hbm()] + [vmem()] * (ring + 1),
        out_shape=[
            pltpu.HBM((lanes, features), bf16),
            *[jax.ShapeDtypeStruct((rows // ring, features), f32)] * ring,
            jax.ShapeDtypeStruct((1, LANES), f32),
        ],
        scratch_shapes=[
            pltpu.VMEM((GROUP * DLEN, CHUNK), f32),
            pltpu.VMEM((GROUP * DLEN, CHUNK), f32),
            pltpu.VMEM(level.shape, f32),
            pltpu.VMEM((lanes, features), bf16),
            pltpu.SemaphoreType.DMA((lanes // CHUNK,)),
        ],
        compiler_params=grant(14),
        name="slopes",
    )(*spans, steep, docs, queries, level, logits, stats)


def head_backward_kernel(x_ref, gain_ref, emb_ref, proj_ref, gq_ref, g0, g1, g2, g3, out_ref,
                         out_vmem, sems):
    pairs = x_ref.shape[0]
    sends = []
    for first in range(0, pairs, TOGETHER):
        group = range(first, first + TOGETHER)
        grads = []
        for p in group:
            at = slice(p * DLEN, (p + 1) * DLEN)
            grad_docs = g0[at] + g1[at] + g2[at] + g3[at]
            grad_query = jnp.sum(gq_ref[:, p * QLEN:(p + 1) * QLEN].astype(f32), axis=0)
            grad_vectors = jnp.concatenate([grad_query, grad_docs], axis=0)
            projected = proj_ref[p]
            inverse_length = lax.rsqrt(
                jnp.sum(projected * projected, axis=-1, keepdims=True) + EPSILON
            )
            unit = projected * inverse_length
            along = jnp.sum(unit * grad_vectors, axis=-1, keepdims=True)
            grads.append((inverse_length * (grad_vectors - unit * along)).astype(bf16))
        normed = dot_nt(jnp.concatenate(grads, axis=0), emb_ref[...])
        rows = normed.shape[0] // TOGETHER
        for n, p in enumerate(group):
            values = x_ref[p].astype(f32)
            inverse_rms = lax.rsqrt(jnp.mean(values * values, axis=-1, keepdims=True) + EPSILON)
            weighted = normed[n * rows:(n + 1) * rows] * gain_ref[...]
            mean_term = jnp.mean(values * weighted, axis=-1, keepdims=True)
            out_vmem[p] = (
                inverse_rms * weighted
                - values * (inverse_rms * inverse_rms * inverse_rms) * mean_term
            ).astype(bf16)
            sends.append(pltpu.make_async_copy(out_vmem.at[p], out_ref.at[p], sems.at[p]))
            sends[-1].start()
    for send in sends:
        send.wait()


def head_backward(x, gain, emb, projected, grad_queries, grad_docs):
    pairs = x.shape[0]
    return pl.pallas_call(
        head_backward_kernel,
        in_specs=[vmem()] * 9,
        out_specs=hbm(),
        out_shape=jax.ShapeDtypeStruct(x.shape, bf16),
        scratch_shapes=[pltpu.VMEM(x.shape, bf16), pltpu.SemaphoreType.DMA((pairs,))],
        compiler_params=grant(14),
        name="head_backward",
    )(x, gain, emb, projected, grad_queries, *grad_docs)


def all_slices(own):
    swap = [(0, 1), (1, 0)]
    ring = lax.axis_size("z")
    mirror = [
        (h * ring + z, (1 - h) * ring + ring - 1 - z) for h in range(2) for z in range(ring)
    ]
    far = lax.ppermute(own, ("h", "z"), mirror)
    core = lax.ppermute(own, "k", swap)
    far_core = lax.ppermute(far, "k", swap)
    return own, core, far, far_core


def traded(array, step):
    return lax.ppermute(array, "z", [(i, i ^ step) for i in range(lax.axis_size("z"))])


def local(x, gain, embedding, request_span, passage_span, matching_pair, steepness):
    x = x[0]
    pairs = x.shape[0]
    ring = lax.axis_size("z")
    gain = gain[None]
    spans = (request_span, passage_span, matching_pair)
    plane = lax.axis_size(PLANE)

    def swapped(blocks):
        return lax.all_to_all(blocks, PLANE, split_axis=0, concat_axis=0, tiled=True)

    normed = normalize(x, gain)
    slices = all_slices(embedding)
    part = project_partly(normed, *slices[:3])
    copies, d, projected = project(normed, part, slices[3], plane)
    emb = assemble(slices)
    docs = [d] + [traded(d, s) for s in range(1, ring)]
    queries = swapped(copies)
    queries = queries.reshape(-1, queries.shape[-1])
    docs, level, logits, stats = scores_forward(spans, steepness, queries, docs, pairs)
    stats = swapped(stats)
    gq, *gd, loss = slopes(
        spans, steepness, docs, queries, level, logits, stats, pairs, ring
    )
    grad_docs = [gd[0]] + [traded(gd[s], s) for s in range(1, ring)]
    grad_queries = swapped(gq.reshape(copies.shape))
    grad_x = head_backward(x, gain, emb, projected, grad_queries, grad_docs)
    own = lax.dynamic_slice_in_dim(loss, plane_index() * pairs, pairs, 1)
    return grad_x[None], own


def solution(mesh):
    side = round(mesh.shape["dp"] ** (1 / 3))
    finer = Mesh(mesh.devices.reshape(2, 2, side, side, side), ("h", "k", "x", "y", "z"))
    rows = P(SECTION, DP, None, None)
    return jax.shard_map(
        local,
        mesh=finer,
        in_specs=(rows, P(), P(SECTION, None), P(), P(), P(), P()),
        out_specs=(rows, P(SECTION, DP)),
        check_vma=False,
    )
```

```python
import functools

import jax
import jax.numpy as jnp
from jax import lax
from jax.experimental import pallas as pl
from jax.experimental.pallas import tpu as pltpu
from jax.sharding import Mesh
from jax.sharding import PartitionSpec as P

QLEN = 32
DLEN = 64
LANES = 128
GROUP = 8
CHUNK = 512
CHUNK_F = 2048
TOGETHER = 4
DLEN_LEAST = 32
SECTION = ("h", "k")
PLANE = ("x", "y")
DP = ("x", "y", "z")

EPSILON = 1e-06
OBJECTIVE_FACTOR = 1024.0
MASKED = -1e30

LOG2_E = 1.4426950408889634
LN_2 = 0.6931471805599453

f32 = jnp.float32
bf16 = jnp.bfloat16


def grant(mib):
    return pltpu.CompilerParams(vmem_limit_bytes=mib * 1024 * 1024)


def vmem():
    return pl.BlockSpec(memory_space=pltpu.VMEM)


def hbm():
    return pl.BlockSpec(memory_space=pltpu.HBM)


def smem():
    return pl.BlockSpec(memory_space=pltpu.SMEM)


def dot_nt(a, b):
    return lax.dot_general(a, b, (((1,), (1,)), ((), ())), preferred_element_type=f32)


def dot_tn(a, b):
    return lax.dot_general(a, b, (((0,), (0,)), ((), ())), preferred_element_type=f32)


def in_turn(blocks, fill, use):
    fill(0, 0)
    for block in range(blocks):
        if block + 1 < blocks:
            fill(block + 1, (block + 1) % 2)
        use(block, block % 2)


def section_index():
    return lax.axis_index("h"), lax.axis_index("k")


def normalize_kernel(x_ref, gain_ref, normed_ref):
    values = x_ref[0].astype(f32)
    inverse_rms = lax.rsqrt(jnp.mean(values * values, axis=-1, keepdims=True) + EPSILON)
    normed_ref[0] = (values * inverse_rms * gain_ref[...]).astype(bf16)


def normalize(x, gain):
    pairs, length, width = x.shape
    rows = pl.BlockSpec((1, length, width), lambda i: (i, 0, 0))
    return pl.pallas_call(
        normalize_kernel,
        grid=(pairs,),
        in_specs=[rows, pl.BlockSpec((1, width), lambda i: (0, 0))],
        out_specs=rows,
        out_shape=jax.ShapeDtypeStruct(x.shape, bf16),
        compiler_params=grant(6),
        name="normalize",
    )(x, gain)


def section_rows(depth, far, other):
    h, k = section_index()
    section = (1 - h if far else h) * 2 + (1 - k if other else k)
    return pl.ds(pl.multiple_of(section * depth, depth), depth)


def partial_kernel(normed_ref, own_ref, core_ref, far_ref, part_ref):
    depth = own_ref.shape[0]
    for p in range(normed_ref.shape[0]):
        part_ref[p] = sum(
            jnp.dot(normed_ref[p, :, section_rows(depth, far, other)], ref[...],
                    preferred_element_type=f32)
            for ref, far, other in ((own_ref, 0, 0), (core_ref, 0, 1), (far_ref, 1, 0))
        )


def project_partly(normed, own, core, far):
    pairs, length, _ = normed.shape
    return pl.pallas_call(
        partial_kernel,
        in_specs=[vmem()] * 4,
        out_specs=vmem(),
        out_shape=jax.ShapeDtypeStruct((pairs, length, own.shape[1]), f32),
        compiler_params=grant(6),
        name="project_partly",
    )(normed, own, core, far)


def project_kernel(normed_ref, part_ref, last_ref, copies_ref, d_ref, proj_ref, q_ref, sems):
    depth = last_ref.shape[0]
    for p in range(normed_ref.shape[0]):
        projected = part_ref[p] + jnp.dot(
            normed_ref[p, :, section_rows(depth, 1, 1)], last_ref[...],
            preferred_element_type=f32,
        )
        inverse_length = lax.rsqrt(
            jnp.sum(projected * projected, axis=-1, keepdims=True) + EPSILON
        )
        vectors = (projected * inverse_length).astype(bf16)
        q_ref[p * QLEN:(p + 1) * QLEN] = vectors[:QLEN]
        d_ref[p * DLEN:(p + 1) * DLEN] = vectors[QLEN:]
        proj_ref[p] = projected
    copies = [
        pltpu.make_async_copy(q_ref, copies_ref.at[n], sems.at[n])
        for n in range(copies_ref.shape[0])
    ]
    for copy in copies:
        copy.start()
    for copy in copies:
        copy.wait()


def project(normed, part, last, readers):
    pairs, length, _ = normed.shape
    features = last.shape[1]
    return pl.pallas_call(
        project_kernel,
        in_specs=[vmem()] * 3,
        out_specs=[hbm(), vmem(), vmem()],
        out_shape=[
            pltpu.HBM((readers, pairs * QLEN, features), bf16),
            jax.ShapeDtypeStruct((pairs * DLEN, features), bf16),
            jax.ShapeDtypeStruct((pairs, length, features), f32),
        ],
        scratch_shapes=[
            pltpu.VMEM((pairs * QLEN, features), bf16),
            pltpu.SemaphoreType.DMA((readers,)),
        ],
        compiler_params=grant(6),
        name="project",
    )(normed, part, last)


def assemble_kernel(own_ref, core_ref, far_ref, far_core_ref, emb_ref):
    depth = own_ref.shape[0]
    emb_ref[section_rows(depth, 0, 0), :] = own_ref[...]
    emb_ref[section_rows(depth, 0, 1), :] = core_ref[...]
    emb_ref[section_rows(depth, 1, 0), :] = far_ref[...]
    emb_ref[section_rows(depth, 1, 1), :] = far_core_ref[...]


def assemble(slices):
    depth, features = slices[0].shape
    return pl.pallas_call(
        assemble_kernel,
        in_specs=[vmem()] * 4,
        out_specs=vmem(),
        out_shape=jax.ShapeDtypeStruct((depth * len(slices), features), bf16),
        compiler_params=grant(4),
        name="assemble",
    )(*slices)


def micro_index():
    h, k = section_index()
    return h * 2 + k


def plane_index():
    return lax.axis_index("x") * lax.axis_size("y") + lax.axis_index("y")


def query_pair(holder, t, pairs):
    return (holder * lax.axis_size("z") + lax.axis_index("z")) * pairs + t


def document_pair(c, pairs):
    z = jnp.bitwise_xor(lax.axis_index("z"), lax.div(c, pairs))
    return (plane_index() * lax.axis_size("z") + z) * pairs + lax.rem(c, pairs)


def query_weights(request_ref, micro, holders, pairs):
    wide = pairs * QLEN
    lane = lax.broadcasted_iota(jnp.int32, (1, wide), 1)
    owner = lax.div(lane, QLEN)
    place = lane - owner * QLEN
    parts = []
    for holder in range(holders):
        span = jnp.zeros((1, wide), jnp.int32)
        for t in range(pairs):
            span = jnp.where(owner == t, request_ref[micro, query_pair(holder, t, pairs)], span)
        live = jnp.where(place < span, 1.0, 0.0).astype(f32)
        parts.append(live / span.astype(f32))
    return jnp.concatenate(parts, axis=1)


def matches(match_ref, micro, holders, pairs):
    lane = lax.broadcasted_iota(jnp.int32, (1, LANES), 1)
    match = jnp.full((1, LANES), -1, jnp.int32)
    for holder in range(holders):
        for t in range(pairs):
            match = jnp.where(
                lane == holder * pairs + t, match_ref[micro, query_pair(holder, t, pairs)], match
            )
    return match


def first_owners():
    start = lax.broadcasted_iota(jnp.int32, (LANES, LANES), 0) * QLEN
    ahead = lax.broadcasted_iota(jnp.int32, (LANES, LANES), 1) - start
    return jnp.where((ahead >= 0) & (ahead < QLEN), 1.0, 0.0).astype(bf16)


def parts_of(values):
    high = values.astype(bf16)
    rest = values - high.astype(f32)
    middle = rest.astype(bf16)
    low = (rest - middle.astype(f32)).astype(bf16)
    return jnp.concatenate([low, middle, high], axis=0)


def joined(parts):
    rows = parts.shape[0] // 3
    return parts[:rows] + parts[rows:2 * rows] + parts[2 * rows:]


def sums_by_query(terms, pairs):
    wide = pairs * QLEN
    owners = first_owners()
    total = None
    for holder in range(terms.shape[1] // wide):
        sums = joined(dot_nt(parts_of(terms[:, holder * wide:(holder + 1) * wide]), owners))
        sums = pltpu.roll(sums, holder * pairs, 1) if holder else sums
        total = sums if total is None else total + sums
    return total


def given_to_tokens(values, holders, pairs):
    owners = first_owners()
    given = []
    for holder in range(holders):
        own = pltpu.roll(values, LANES - holder * pairs, 1) if holder else values
        given.append(joined(jnp.dot(parts_of(own), owners, preferred_element_type=f32)))
    return jnp.concatenate(given, axis=1)


def prepare_kernel(pairs, request_ref, passage_ref, match_ref, steep_ref,
                   weight_ref, match_out, span_ref, scale_ref):
    micro = micro_index()
    holders = weight_ref.shape[1] // (pairs * QLEN)
    weight_ref[...] = query_weights(request_ref, micro, holders, pairs)
    match_out[...] = matches(match_ref, micro, holders, pairs)
    count = span_ref.shape[0]
    place = lax.broadcasted_iota(jnp.int32, (count, LANES), 0)
    spans = jnp.zeros((count, LANES), jnp.int32)
    for c in range(count):
        spans = jnp.where(place == c, passage_ref[micro, document_pair(c, pairs)], spans)
    span_ref[...] = spans
    row = lax.broadcasted_iota(jnp.int32, scale_ref.shape, 0)
    beta = jnp.full(scale_ref.shape, steep_ref[0], f32)
    mult = jnp.full(scale_ref.shape, steep_ref[1], f32)
    scale_ref[...] = jnp.where(row == 0, beta * LOG2_E, jnp.where(row == 1, mult, LN_2 / beta))


def prepare(spans, steep, holders, pairs, ring):
    return pl.pallas_call(
        functools.partial(prepare_kernel, pairs),
        in_specs=[smem()] * 4,
        out_specs=[vmem()] * 4,
        out_shape=[
            jax.ShapeDtypeStruct((1, holders * pairs * QLEN), f32),
            jax.ShapeDtypeStruct((1, LANES), jnp.int32),
            jax.ShapeDtypeStruct((ring * pairs, LANES), jnp.int32),
            jax.ShapeDtypeStruct((8, LANES), f32),
        ],
        compiler_params=grant(2),
        name="prepare",
    )(*spans, steep)


def across(row, lanes):
    return jnp.concatenate([row] * (lanes // LANES), axis=1)


def scores_kernel(pairs, weight_ref, match_ref, span_ref, scale_ref,
                  q_all, d0, d1, d2, d3,
                  docs_ref, level_ref, logits_ref, stats_ref, sim_a, sim_b):
    beta2 = across(scale_ref[0:1], CHUNK_F)
    arrived = (d0, d1, d2, d3)
    own = d0.shape[0]
    for n, ref in enumerate(arrived):
        docs_ref[n * own:(n + 1) * own, :] = ref[...]
    lanes = q_all.shape[0]
    count = docs_ref.shape[0] // DLEN
    rows = GROUP * DLEN
    sims = (sim_a, sim_b)
    halves = count // GROUP
    token = lax.broadcasted_iota(jnp.int32, (DLEN - DLEN_LEAST, 1), 0) + DLEN_LEAST

    def spot(block):
        half, chunk = block % halves, block // halves
        return half * GROUP, slice(chunk * CHUNK_F, (chunk + 1) * CHUNK_F)

    def similarity(block, slot):
        c, at = spot(block)
        sims[slot][...] = dot_nt(docs_ref[c * DLEN:c * DLEN + rows, :], q_all[at, :])

    def pool(block, slot):
        ref = sims[slot]
        c, at = spot(block)
        levels = []
        for n in range(GROUP):
            span = across(span_ref[c + n:c + n + 1], CHUNK_F)
            row = n * DLEN
            early = ref[row:row + DLEN_LEAST, :]
            late = jnp.where(token < span, ref[row + DLEN_LEAST:row + DLEN, :], MASKED)
            highest = jnp.max(jnp.maximum(early, late), axis=0, keepdims=True)
            total = jnp.sum(
                jnp.exp2(beta2 * (early - highest)) + jnp.exp2(beta2 * (late - highest)),
                axis=0,
                keepdims=True,
            )
            levels.append(beta2 * highest + jnp.log2(total))
        level_ref[c:c + GROUP, at] = jnp.concatenate(levels, axis=0)

    in_turn(halves * (lanes // CHUNK_F), similarity, pool)

    holders = lanes // (pairs * QLEN)
    smooth = level_ref[...] * across(scale_ref[2:3], lanes)
    logits = scale_ref[1:2] * sums_by_query(smooth * weight_ref[...], pairs)
    logits_ref[...] = logits
    column = document_pair(lax.broadcasted_iota(jnp.int32, (count, 1), 0), pairs)
    match = match_ref[...]
    highest = jnp.max(logits, axis=0, keepdims=True)
    local = highest + jnp.log(jnp.sum(jnp.exp(logits - highest), axis=0, keepdims=True))
    positive = jnp.sum(jnp.where(column == match, logits, 0.0), axis=0, keepdims=True)
    tile = jnp.concatenate([local, positive, jnp.zeros((6, LANES), f32)], axis=0)
    for holder in range(holders):
        stats_ref[holder] = tile


def scores_forward(prepared, queries, docs, pairs):
    lanes, features = queries.shape
    rows = docs[0].shape[0] * len(docs)
    count = rows // DLEN
    holders = lanes // (pairs * QLEN)
    return pl.pallas_call(
        functools.partial(scores_kernel, pairs),
        in_specs=[vmem()] * 9,
        out_specs=[vmem()] * 4,
        out_shape=[
            jax.ShapeDtypeStruct((rows, features), bf16),
            jax.ShapeDtypeStruct((count, lanes), f32),
            jax.ShapeDtypeStruct((count, LANES), f32),
            jax.ShapeDtypeStruct((holders, 8, LANES), f32),
        ],
        scratch_shapes=[
            pltpu.VMEM((GROUP * DLEN, CHUNK_F), f32),
            pltpu.VMEM((GROUP * DLEN, CHUNK_F), f32),
        ],
        compiler_params=grant(10),
        name="scores_forward",
    )(*prepared, queries, *docs)


def slopes_kernel(pairs, weight_ref, match_ref, span_ref, scale_ref,
                  docs_ref, q_all, level_ref, logits_ref, stats_ref,
                  gq_ref, gd0, gd1, gd2, gd3, loss_ref,
                  sim_a, sim_b, coef_ref, gq_vmem, sems):
    beta2 = across(scale_ref[0:1], CHUNK)
    lanes = q_all.shape[0]
    count = docs_ref.shape[0] // DLEN
    rows = GROUP * DLEN
    sims = (sim_a, sim_b)
    halves = count // GROUP
    holders = lanes // (pairs * QLEN)

    stats = stats_ref[...]
    locals_ = stats[:, 0, :]
    highest = jnp.max(locals_, axis=0, keepdims=True)
    log_total = highest + jnp.log(jnp.sum(jnp.exp(locals_ - highest), axis=0, keepdims=True))
    loss_ref[...] = log_total - jnp.sum(stats[:, 1, :], axis=0, keepdims=True)

    column = document_pair(lax.broadcasted_iota(jnp.int32, (count, 1), 0), pairs)
    match = match_ref[...]
    share = jnp.exp(logits_ref[...] - log_total) - jnp.where(column == match, 1.0, 0.0)
    slope = given_to_tokens(OBJECTIVE_FACTOR * scale_ref[1:2] * share, holders, pairs)
    coef_ref[...] = weight_ref[...] * slope

    token = lax.broadcasted_iota(jnp.int32, (DLEN - DLEN_LEAST, 1), 0) + DLEN_LEAST
    turned_parts = []
    sends = []
    gds = (gd0, gd1, gd2, gd3)
    own = gd0.shape[0]

    def spot(block):
        half, chunk = block % halves, block // halves
        return half * GROUP, slice(chunk * CHUNK, (chunk + 1) * CHUNK)

    def similarity(block, slot):
        c, at = spot(block)
        sims[slot][...] = dot_nt(docs_ref[c * DLEN:c * DLEN + rows, :], q_all[at, :])

    def weigh(block, slot):
        ref = sims[slot]
        c, at = spot(block)
        parts = []
        for n in range(GROUP):
            live = across(span_ref[c + n:c + n + 1], CHUNK)
            level = level_ref[c + n:c + n + 1, at]
            coef = coef_ref[c + n:c + n + 1, at]
            row = n * DLEN
            share = jnp.exp2(beta2 * ref[row:row + DLEN_LEAST, :] - level)
            parts.append((coef * share).astype(bf16))
            share = jnp.exp2(beta2 * ref[row + DLEN_LEAST:row + DLEN, :] - level)
            parts.append(jnp.where(token < live, coef * share, 0.0).astype(bf16))
        grad = jnp.concatenate(parts, axis=0)
        here = slice(c * DLEN, c * DLEN + rows)
        product = jnp.dot(grad, q_all[at, :], preferred_element_type=f32)
        for n in range(rows // own):
            ref = gds[c * DLEN // own + n]
            part = product[n * own:(n + 1) * own]
            ref[...] = part if block < halves else ref[...] + part
        turned_parts.append(dot_tn(docs_ref[here, :], grad))
        if len(turned_parts) == halves:
            total = functools.reduce(jnp.add, turned_parts)
            turned_parts.clear()
            gq_vmem[at, :] = total.T.astype(gq_vmem.dtype)
            send = pltpu.make_async_copy(
                gq_vmem.at[at], gq_ref.at[at], sems.at[block // halves]
            )
            send.start()
            sends.append(send)

    in_turn(halves * (lanes // CHUNK), similarity, weigh)
    for send in sends:
        send.wait()


def slopes(prepared, docs, queries, level, logits, stats, pairs, ring):
    lanes, features = queries.shape
    rows = docs.shape[0]
    return pl.pallas_call(
        functools.partial(slopes_kernel, pairs),
        in_specs=[vmem()] * 9,
        out_specs=[hbm()] + [vmem()] * (ring + 1),
        out_shape=[
            pltpu.HBM((lanes, features), bf16),
            *[jax.ShapeDtypeStruct((rows // ring, features), f32)] * ring,
            jax.ShapeDtypeStruct((1, LANES), f32),
        ],
        scratch_shapes=[
            pltpu.VMEM((GROUP * DLEN, CHUNK), f32),
            pltpu.VMEM((GROUP * DLEN, CHUNK), f32),
            pltpu.VMEM(level.shape, f32),
            pltpu.VMEM((lanes, features), bf16),
            pltpu.SemaphoreType.DMA((lanes // CHUNK,)),
        ],
        compiler_params=grant(14),
        name="slopes",
    )(*prepared, docs, queries, level, logits, stats)


def head_backward_kernel(x_ref, gain_ref, emb_ref, proj_ref, gq_ref, g0, g1, g2, g3, out_ref,
                         out_vmem, sems):
    pairs = x_ref.shape[0]
    sends = []
    for first in range(0, pairs, TOGETHER):
        group = range(first, first + TOGETHER)
        grads = []
        for p in group:
            at = slice(p * DLEN, (p + 1) * DLEN)
            grad_docs = g0[at] + g1[at] + g2[at] + g3[at]
            grad_query = jnp.sum(gq_ref[:, p * QLEN:(p + 1) * QLEN].astype(f32), axis=0)
            grad_vectors = jnp.concatenate([grad_query, grad_docs], axis=0)
            projected = proj_ref[p]
            inverse_length = lax.rsqrt(
                jnp.sum(projected * projected, axis=-1, keepdims=True) + EPSILON
            )
            unit = projected * inverse_length
            along = jnp.sum(unit * grad_vectors, axis=-1, keepdims=True)
            grads.append((inverse_length * (grad_vectors - unit * along)).astype(bf16))
        normed = dot_nt(jnp.concatenate(grads, axis=0), emb_ref[...])
        rows = normed.shape[0] // TOGETHER
        for n, p in enumerate(group):
            values = x_ref[p].astype(f32)
            inverse_rms = lax.rsqrt(jnp.mean(values * values, axis=-1, keepdims=True) + EPSILON)
            weighted = normed[n * rows:(n + 1) * rows] * gain_ref[...]
            mean_term = jnp.mean(values * weighted, axis=-1, keepdims=True)
            out_vmem[p] = (
                inverse_rms * weighted
                - values * (inverse_rms * inverse_rms * inverse_rms * mean_term)
            ).astype(bf16)
            sends.append(pltpu.make_async_copy(out_vmem.at[p], out_ref.at[p], sems.at[p]))
            sends[-1].start()
    for send in sends:
        send.wait()


def head_backward(x, gain, emb, projected, grad_queries, grad_docs):
    pairs = x.shape[0]
    return pl.pallas_call(
        head_backward_kernel,
        in_specs=[vmem()] * 9,
        out_specs=hbm(),
        out_shape=jax.ShapeDtypeStruct(x.shape, bf16),
        scratch_shapes=[pltpu.VMEM(x.shape, bf16), pltpu.SemaphoreType.DMA((pairs,))],
        compiler_params=grant(14),
        name="head_backward",
    )(x, gain, emb, projected, grad_queries, *grad_docs)


def all_slices(own):
    swap = [(0, 1), (1, 0)]
    ring = lax.axis_size("z")
    mirror = [
        (h * ring + z, (1 - h) * ring + ring - 1 - z) for h in range(2) for z in range(ring)
    ]
    far = lax.ppermute(own, ("h", "z"), mirror)
    core = lax.ppermute(own, "k", swap)
    far_core = lax.ppermute(far, "k", swap)
    return own, core, far, far_core


def traded(array, step):
    return lax.ppermute(array, "z", [(i, i ^ step) for i in range(lax.axis_size("z"))])


def local(x, gain, embedding, request_span, passage_span, matching_pair, steepness):
    x = x[0]
    pairs = x.shape[0]
    ring = lax.axis_size("z")
    gain = gain[None]
    spans = (request_span, passage_span, matching_pair)
    plane = lax.axis_size(PLANE)

    def swapped(blocks):
        return lax.all_to_all(blocks, PLANE, split_axis=0, concat_axis=0, tiled=True)

    normed = normalize(x, gain)
    slices = all_slices(embedding)
    part = project_partly(normed, *slices[:3])
    copies, d, projected = project(normed, part, slices[3], plane)
    emb = assemble(slices)
    prepared = prepare(spans, steepness, plane, pairs, ring)
    docs = [d] + [traded(d, s) for s in range(1, ring)]
    queries = swapped(copies)
    queries = queries.reshape(-1, queries.shape[-1])
    docs, level, logits, stats = scores_forward(prepared, queries, docs, pairs)
    stats = swapped(stats)
    gq, *gd, loss = slopes(
        prepared, docs, queries, level, logits, stats, pairs, ring
    )
    grad_docs = [gd[0]] + [traded(gd[s], s) for s in range(1, ring)]
    grad_queries = swapped(gq.reshape(copies.shape))
    grad_x = head_backward(x, gain, emb, projected, grad_queries, grad_docs)
    own = lax.dynamic_slice_in_dim(loss, plane_index() * pairs, pairs, 1)
    return grad_x[None], own


def solution(mesh):
    side = round(mesh.shape["dp"] ** (1 / 3))
    finer = Mesh(mesh.devices.reshape(2, 2, side, side, side), ("h", "k", "x", "y", "z"))
    rows = P(SECTION, DP, None, None)
    return jax.shard_map(
        local,
        mesh=finer,
        in_specs=(rows, P(), P(SECTION, None), P(), P(), P(), P()),
        out_specs=(rows, P(SECTION, DP)),
        check_vma=False,
    )
```
